128 devices in a mesh: expert: 4 (over x_lo, core), shard: 32 (over z, y, x_hi).
Axes of the slice: x: 4 (x_hi: 2, x_lo: 2; x = x_hi * 2 + x_lo), y: 4, z: 4, core: 2. Of those that a mesh axis runs over, the one named last changes fastest.
Arguments:
- master_gate: float32 [64, 2048, 1024], P('expert', 'shard'), may hold values from -0.25 to 0.25
- second_gate: bfloat16 [64, 2048, 1024], P('expert', 'shard'), may hold values from -0.0625 to 0.0625
- master_up: float32 [64, 2048, 1024], P('expert', 'shard'), may hold values from -0.25 to 0.25
- second_up: bfloat16 [64, 2048, 1024], P('expert', 'shard'), may hold values from -0.0625 to 0.0625
- master_down: float32 [64, 1024, 2048], P('expert', None, 'shard'), may hold values from -0.375 to 0.375
- second_down: bfloat16 [64, 1024, 2048], P('expert', None, 'shard'), may hold values from -0.09375 to 0.09375
- router_weight: float32 [2048, 64], P('shard', 'expert'), may hold values from -0.125 to 0.125
- router_gain: float32 [2048], P('shard'), may hold values from 0.25 to 1.75
Outputs:
- final_gate: bfloat16 [64, 2048, 1024], P('expert', None, 'shard')
- final_up: bfloat16 [64, 2048, 1024], P('expert', None, 'shard')
- final_down: bfloat16 [64, 1024, 2048], P('expert', 'shard')
- scale_gate: float32 [64, 1024], P('expert', 'shard')
- scale_up: float32 [64, 1024], P('expert', 'shard')
- scale_down: float32 [64, 1024], P('expert', 'shard')
- serve_router: bfloat16 [2048, 64], replicated
The draws below stay inside these ranges and needn't reach their ends.
All inputs are finite; a program needn't handle non-finite values. Where the reference program divides by a largest or mean magnitude, that divisor is 1e-20 or more.
Results may differ from the reference program's by a relative error of at most 0.001.
Values may be sent and summed in bfloat16 or wider, within the bound.
A program may use at most 128 MiB of HBM per device.

```python
import jax
import jax.numpy as jnp

EXPERTS = 64
D_MODEL = 2048
D_EXPERT = 1024


def raised(result, key, source, target, parts, factor):
    owner, partner = [(jnp.arange(result.shape[position]) // (result.shape[position] // parts)).reshape([-1 if axis == position else 1 for axis in range(result.ndim)]) for position in (source, target)]
    chosen = jax.random.permutation(key, parts)[partner]
    strong = (owner == chosen) | (owner == (partner + parts // 2) % parts)
    return jnp.where(strong, factor * result, result)


def shard_levels(rng, shape, split, low, largest):
    factor_of, own = 1.0, jax.random.fold_in(rng, 6)
    for position, blocks in split:
        heights = jnp.exp(jax.random.uniform(jax.random.fold_in(own, position), (blocks,), jnp.float32, low / len(split), largest / len(split)))
        factor_of = factor_of * jnp.repeat(heights, shape[position] // blocks).reshape([-1 if axis == position else 1 for axis in range(len(shape))])
    return factor_of


def normal_values(rng, dims, scale, bound, cuts=(), held_as=jnp.bfloat16):
    gain = shard_levels(rng, dims, cuts, -0.22, 0.18) if cuts else 1.0
    entries = jax.random.normal(rng, dims, jnp.float32) * scale * gain
    return jnp.minimum(jnp.maximum(entries, -bound), bound).astype(held_as)


def gaussian_with(key, dims, width, bound, cuts, heavy, dtype=jnp.bfloat16):
    values = width * jax.random.normal(key, dims, jnp.float32)
    if cuts:
        values = values * shard_levels(key, dims, cuts, -0.22, 0.18)
    return jnp.clip(raised(values, jax.random.fold_in(key, 3), *heavy), -bound, bound).astype(dtype)


def setup_inputs(seed: int = 0) -> dict:
    keys = jax.random.split(jax.random.key(seed), 9)
    master_gate = gaussian_with(keys[0], (EXPERTS, D_MODEL, D_EXPERT), D_MODEL ** -0.5, 0.25, ((0, 4), (1, 32)), (1, 2, 32, 2.75), jnp.float32)
    second_gate = normal_values(keys[1], (EXPERTS, D_MODEL, D_EXPERT), (D_MODEL * 4) ** -0.5, 0.0625, ((0, 4), (1, 32)))
    master_up = gaussian_with(keys[2], (EXPERTS, D_MODEL, D_EXPERT), D_MODEL ** -0.5, 0.25, ((0, 4), (1, 32)), (1, 2, 32, 2.75), jnp.float32)
    second_up = normal_values(keys[3], (EXPERTS, D_MODEL, D_EXPERT), (D_MODEL * 4) ** -0.5, 0.0625, ((0, 4), (1, 32)))
    master_down = gaussian_with(keys[4], (EXPERTS, D_EXPERT, D_MODEL), D_EXPERT ** -0.5, 0.375, ((0, 4), (2, 32)), (2, 1, 32, 2.75), jnp.float32)
    second_down = normal_values(keys[5], (EXPERTS, D_EXPERT, D_MODEL), (D_EXPERT * 4) ** -0.5, 0.09375, ((0, 4), (2, 32)))
    router_weight = normal_values(keys[6], (D_MODEL, EXPERTS), D_MODEL ** -0.5, 0.125, ((0, 32), (1, 4)), jnp.float32)
    router_gain = jnp.clip(1.0 + 0.15 * jax.random.normal(keys[7], (D_MODEL,), jnp.float32), 0.25, 1.75)
    return {"master_gate": master_gate, "second_gate": second_gate, "master_up": master_up, "second_up": second_up, "master_down": master_down, "second_down": second_down, "router_weight": router_weight, "router_gain": router_gain}


def reference(master_gate, second_gate, master_up, second_up, master_down, second_down, router_weight, router_gain):
    merged_gate = master_gate + second_gate.astype(jnp.float32)
    merged_up = master_up + second_up.astype(jnp.float32)
    merged_down = master_down + second_down.astype(jnp.float32)
    scale_gate = jnp.max(jnp.abs(merged_gate), axis=1)
    final_gate = (merged_gate / jnp.expand_dims(scale_gate, 1)).astype(jnp.bfloat16)
    scale_up = jnp.max(jnp.abs(merged_up), axis=1)
    final_up = (merged_up / jnp.expand_dims(scale_up, 1)).astype(jnp.bfloat16)
    scale_down = jnp.max(jnp.abs(merged_down), axis=2)
    final_down = (merged_down / jnp.expand_dims(scale_down, 2)).astype(jnp.bfloat16)
    serve_router = (router_weight * router_gain[:, None]).astype(jnp.bfloat16)
    return final_gate, final_up, final_down, scale_gate, scale_up, scale_down, serve_router
```

```python
import jax
import jax.numpy as jnp
from jax import lax
from jax.experimental import pallas as pl
from jax.experimental.pallas import tpu as pltpu
from jax.sharding import PartitionSpec as P

MESH = pl.DeviceIdType.MESH
F32, BF16 = jnp.float32, jnp.bfloat16
N = 32
E, R, C = 16, 64, 1024
W = C // N
GE = 4
NG = E // GE
OFFSETS = [
    (dx, dy, dz) for dx in range(2) for dy in range(4) for dz in range(4) if (dx, dy, dz) != (0, 0, 0)
]


def kernel(
    mg, sg, mu, su, md, sd, rw, rg,
    og, ou, od, cg, cu, cd, orr,
    mbuf, sbuf, lmax, rs_s, rs_r, ag_s, ag_r, inv, snd, rcv, rt_s, rt_r, rt_x,
    load_sem, rs_ss, rs_rs, ag_ss, ag_rs, d_ss, d_rs, rt_ss, rt_rs, rx_ss, rx_rs,
):
    e_id = lax.axis_index("expert")
    me = lax.axis_index("shard")
    xhi = lax.rem(me, 2)
    y = lax.rem(me // 2, 4)
    z = me // 8

    masters, seconds = (mg, mu, md), (sg, su, sd)
    for m in range(3):
        for g in range(NG):
            es = pl.ds(g * GE, GE)
            pltpu.make_async_copy(masters[m].at[es], mbuf.at[m, es], load_sem.at[0, m * NG + g]).start()
            pltpu.make_async_copy(seconds[m].at[es], sbuf.at[m, es], load_sem.at[1, m * NG + g]).start()

    peers = []
    for dx, dy, dz in OFFSETS:
        peers.append((lax.rem(z + dz, 4) * 4 + lax.rem(y + dy, 4)) * 2 + lax.rem(xhi + dx, 2))
    mates = [lax.rem(e_id + k, 4) for k in range(1, 4)]

    barrier = pltpu.get_barrier_semaphore()
    for p in peers:
        pl.semaphore_signal(barrier, inc=1, device_id=(e_id, p), device_id_type=MESH)
    for q in mates:
        pl.semaphore_signal(barrier, inc=1, device_id=(q, me), device_id_type=MESH)

    def send_all(src_of, dst, ss, rs):
        for p in peers:
            pltpu.make_async_remote_copy(
                src_ref=src_of(p), dst_ref=dst, send_sem=ss, recv_sem=rs,
                device_id=(e_id, p), device_id_type=MESH,
            ).start()

    def wait_bytes(ref, sem):
        pltpu.make_async_copy(ref, ref, sem).wait()

    rt = rw[...] * rg[...]
    rt_s[...] = jnp.concatenate([rt[:8], rt[8:]], axis=1).astype(BF16)

    def merge(m):
        def group(g, _):
            es = pl.ds(g * GE, GE)
            wait_bytes(mbuf.at[m, es], load_sem.at[0, m * NG + g])
            wait_bytes(sbuf.at[m, es], load_sem.at[1, m * NG + g])

            def one(i, _):
                e = g * GE + i
                x = mbuf[m, e] + sbuf[m, e].astype(F32)
                mbuf[m, e] = x
                lmax[m, pl.ds(e, 1), :] = jnp.max(jnp.abs(x), axis=0, keepdims=True)
                return 0

            lax.fori_loop(0, GE, one, 0)
            return 0

        lax.fori_loop(0, NG, group, 0)
        for t in range(8):
            for q in range(4):
                rs_s[m, 4 * t + q] = jnp.concatenate(
                    [lmax[m, pl.ds(4 * k, 4), pl.ds(128 * t, 128)][:, 32 * q : 32 * q + 32] for k in range(4)], axis=1
                )

    def start_rs(m):
        send_all(lambda p: rs_s.at[m, p], rs_r.at[m, me], rs_ss.at[m], rs_rs.at[m])
        rs_r[m, me] = rs_s[m, me]

    scales = (cg, cu, cd)

    def finish_rs(m):
        wait_bytes(rs_r.at[m, pl.ds(0, N - 1)], rs_rs.at[m])
        top = jnp.max(rs_r[m], axis=0)
        ag_s[m] = top
        ag_r[m, me] = top
        for k in range(4):
            scales[m][pl.ds(4 * k, 4), :] = top[:, 32 * k : 32 * k + 32]
        send_all(lambda p: ag_s.at[m], ag_r.at[m, me], ag_ss.at[m], ag_rs.at[m])

    def finish_ag(m):
        wait_bytes(ag_r.at[m, pl.ds(0, N - 1)], ag_rs.at[m])
        for t in range(8):
            for k in range(4):
                row = jnp.concatenate([ag_r[m, 4 * t + q][:, 32 * k : 32 * k + 32] for q in range(4)], axis=1)
                row = 1.0 / row
                for i in range(4):
                    inv[m, 4 * k + i, :, pl.ds(128 * t, 128)] = row[i : i + 1]

    def send_group(m, g):
        gi = m * NG + g

        def pair(j, _):
            ea = g * GE + 2 * j + xhi
            eb = g * GE + 2 * j + 1 - xhi
            for t in range(8):
                cs = pl.ds(128 * t, 128)
                a = mbuf[m, ea, :, cs] * inv[m, ea, :, cs]
                b = mbuf[m, eb, :, cs] * inv[m, eb, :, cs]
                x = jnp.concatenate([a, b], axis=0).T.astype(BF16)
                snd[gi, pl.ds(4 * t, 4), j] = x.reshape(4, W, 128)
            return 0

        lax.fori_loop(0, GE // 2, pair, 0)
        send_all(lambda p: snd.at[gi, p], rcv.at[gi, me], d_ss.at[gi], d_rs.at[gi])
        rcv[gi, me] = snd[gi, me]

    outs = (og, ou, od)
    low = lax.broadcasted_iota(jnp.int32, (W, 128), 1) < 64

    def receive_group(m, g):
        gi = m * NG + g
        wait_bytes(rcv.at[gi, pl.ds(0, N - 1)], d_rs.at[gi])

        def tile(t, _):
            lanes = pl.ds(pl.multiple_of(t * 128, 128), 128)
            for j in range(GE // 2):
                a = rcv[gi, 2 * t, j].astype(F32)
                b = rcv[gi, 2 * t + 1, j].astype(F32)
                first = jnp.where(low, a, b)
                second = pltpu.roll(jnp.where(low, b, a), 64, 1)
                outs[m][g * GE + 2 * j, :, lanes] = first.astype(BF16)
                outs[m][g * GE + 2 * j + 1, :, lanes] = second.astype(BF16)
            return 0

        lax.fori_loop(0, N // 2, tile, 0)

    merge(0)
    pl.semaphore_wait(barrier, len(peers) + len(mates))
    start_rs(0)
    send_all(lambda p: rt_s, rt_r.at[me], rt_ss, rt_rs)
    rt_r[me] = rt_s[...]
    merge(1)
    start_rs(1)
    merge(2)
    start_rs(2)
    finish_rs(0)
    finish_rs(1)
    finish_rs(2)
    for m in range(3):
        finish_ag(m)

        def go(g, _):
            send_group(m, g)
            return 0

        lax.fori_loop(0, NG, go, 0)
        if m == 0:
            wait_bytes(rt_r.at[pl.ds(0, N - 1)], rt_rs)
            for t in range(16):
                a, b = rt_r[2 * t].astype(F32), rt_r[2 * t + 1].astype(F32)
                top = jnp.concatenate([a[:, :64], b[:, :64]], axis=1)
                bot = jnp.concatenate([a[:, 64:], b[:, 64:]], axis=1)
                rt_x[e_id, :, pl.ds(128 * t, 128)] = jnp.concatenate([top, bot], axis=0).astype(BF16)
            for i, q in enumerate(mates):
                pltpu.make_async_remote_copy(
                    src_ref=rt_x.at[e_id], dst_ref=rt_x.at[e_id], send_sem=rx_ss, recv_sem=rx_rs.at[i],
                    device_id=(q, me), device_id_type=MESH,
                ).start()
    for m in range(3):

        def come(g, _):
            receive_group(m, g)
            return 0

        lax.fori_loop(0, NG, come, 0)
        if m == 0:
            for i in range(3):
                wait_bytes(rt_x.at[0], rx_rs.at[i])
            for k in range(4):
                orr[pl.ds(16 * k, 16), :] = rt_x[k]
    wait_bytes(rt_x.at[pl.ds(0, 3)], rx_ss)
    wait_bytes(rt_r.at[pl.ds(0, N - 1)], rt_ss)
    for m in range(3):
        wait_bytes(rs_r.at[m, pl.ds(0, N - 1)], rs_ss.at[m])
        wait_bytes(ag_r.at[m, pl.ds(0, N - 1)], ag_ss.at[m])

    def drained(gi, _):
        wait_bytes(rcv.at[gi, pl.ds(0, N - 1)], d_ss.at[gi])
        return 0

    lax.fori_loop(0, 3 * NG, drained, 0)


def per_device(
    master_gate, second_gate, master_up, second_up, master_down, second_down, router_weight, router_gain
):
    vmem = pl.BlockSpec(memory_space=pltpu.VMEM)
    hbm = pl.BlockSpec(memory_space=pl.ANY)
    dma = pltpu.SemaphoreType.DMA
    big = jax.ShapeDtypeStruct((E, W, N * R), BF16)
    small = jax.ShapeDtypeStruct((E, W), F32)
    gate, up, down, cg, cu, cd, router = pl.pallas_call(
        kernel,
        out_shape=(big, big, big, small, small, small, jax.ShapeDtypeStruct((4 * E, N * R), BF16)),
        in_specs=[hbm] * 6 + [vmem] * 2,
        out_specs=(vmem,) * 7,
        scratch_shapes=[
            pltpu.VMEM((3, E, R, C), F32),
            pltpu.VMEM((3, E, R, C), BF16),
            pltpu.VMEM((3, E, C), F32),
            pltpu.VMEM((3, N, 4, 128), F32),
            pltpu.VMEM((3, N, 4, 128), F32),
            pltpu.VMEM((3, 4, 128), F32),
            pltpu.VMEM((3, N, 4, 128), F32),
            pltpu.VMEM((3, E, 1, C), F32),
            pltpu.VMEM((3 * NG, N, GE // 2, W, 128), BF16),
            pltpu.VMEM((3 * NG, N, GE // 2, W, 128), BF16),
            pltpu.VMEM((8, 128), BF16),
            pltpu.VMEM((N, 8, 128), BF16),
            pltpu.VMEM((4, 16, N * R), BF16),
            dma((2, 3 * NG)), dma((3,)), dma((3,)), dma((3,)), dma((3,)), dma((3 * NG,)), dma((3 * NG,)),
            dma, dma, dma, dma((3,)),
        ],
        compiler_params=pltpu.CompilerParams(
            collective_id=0, has_side_effects=True, vmem_limit_bytes=62 * 2**20
        ),
        name="reshard",
    )(
        master_gate, second_gate, master_up, second_up,
        jnp.swapaxes(master_down, 1, 2), jnp.swapaxes(second_down, 1, 2),
        router_weight.T, router_gain[None, :],
    )
    return (jnp.swapaxes(gate, 1, 2), jnp.swapaxes(up, 1, 2), down, cg, cu, cd, router.T)


def solution(mesh):
    wide, tall = P("expert", "shard", None), P("expert", None, "shard")
    return jax.shard_map(
        per_device,
        mesh=mesh,
        in_specs=(wide, wide, wide, wide, tall, tall, P("shard", "expert"), P("shard")),
        out_specs=(tall, tall, wide, P("expert", "shard"), P("expert", "shard"), P("expert", "shard"), P()),
        check_vma=False,
    )
```

```python
import jax
import jax.numpy as jnp
from jax import lax
from jax.experimental import pallas as pl
from jax.experimental.pallas import tpu as pltpu
from jax.sharding import PartitionSpec as P

MESH = pl.DeviceIdType.MESH
F32, BF16 = jnp.float32, jnp.bfloat16
N = 32
E, R, C = 16, 64, 1024
W = C // N
GE = 4
NG = E // GE
TOP = 2.0 ** (127 / 16)
TINY = 1e-30
SMALL = 2.0**-126
OFFSETS = [
    (dx, dy, dz) for dx in range(2) for dy in range(4) for dz in range(4) if (dx, dy, dz) != (0, 0, 0)
]


def kernel(
    mg, sg, mu, su, md, sd, rw, rg,
    og, ou, od, cg, cu, cd, orr,
    rwb, rgb, mbuf, sbuf, lmax, inl, fac, rs_s, rs_r, ag_s, ag_r, inv, snd, rcv, rt_s, rt_r, rt_x,
    load_sem, rt_ld, rs_ss, rs_rs, ag_ss, ag_rs, d_ss, d_rs, rt_ss, rt_rs, rx_ss, rx_rs,
):
    e_id = lax.axis_index("expert")
    me = lax.axis_index("shard")
    xhi = lax.rem(me, 2)
    y = lax.rem(me // 2, 4)
    z = me // 8

    masters, seconds = (mg, mu, md), (sg, su, sd)
    for m in range(3):
        for g in range(NG):
            es = pl.ds(g * GE, GE)
            pltpu.make_async_copy(masters[m].at[es], mbuf.at[m, es], load_sem.at[0, m * NG + g]).start()
            pltpu.make_async_copy(seconds[m].at[es], sbuf.at[m, es], load_sem.at[1, m * NG + g]).start()

    peers = []
    for dx, dy, dz in OFFSETS:
        peers.append((lax.rem(z + dz, 4) * 4 + lax.rem(y + dy, 4)) * 2 + lax.rem(xhi + dx, 2))
    core = lax.rem(e_id, 2)
    xlo = e_id // 2
    other = (1 - xlo) * 2 + core
    column = me - xhi
    partner = (xlo * 2 + 1 - core, me)
    right = (other, column + lax.rem(xhi + xlo, 2))
    left = (other, column + lax.rem(xhi + 1 - xlo, 2))
    mates = (partner, right, left)

    barrier = pltpu.get_barrier_semaphore()
    for p in peers:
        pl.semaphore_signal(barrier, inc=1, device_id=(e_id, p), device_id_type=MESH)
    for q in mates:
        pl.semaphore_signal(barrier, inc=1, device_id=q, device_id_type=MESH)

    def send_all(src_of, dst, ss, rs):
        for p in peers:
            pltpu.make_async_remote_copy(
                src_ref=src_of(p), dst_ref=dst, send_sem=ss, recv_sem=rs,
                device_id=(e_id, p), device_id_type=MESH,
            ).start()

    def hop(ref, ss, rs, to):
        return pltpu.make_async_remote_copy(
            src_ref=ref, dst_ref=ref, send_sem=ss, recv_sem=rs, device_id=to, device_id_type=MESH
        )

    def wait_bytes(ref, sem):
        pltpu.make_async_copy(ref, ref, sem).wait()

    router_in = [pltpu.make_async_copy(a, b, rt_ld.at[i]) for i, (a, b) in enumerate(((rw, rwb), (rg, rgb)))]
    for c in router_in:
        c.start()

    def merge(m):
        def group(g, _):
            es = pl.ds(g * GE, GE)
            wait_bytes(mbuf.at[m, es], load_sem.at[0, m * NG + g])
            wait_bytes(sbuf.at[m, es], load_sem.at[1, m * NG + g])

            def one(i, _):
                e = g * GE + i
                x = mbuf[m, e] + sbuf[m, e].astype(F32)
                mbuf[m, e] = x
                lmax[m, pl.ds(e, 1), :] = jnp.max(jnp.abs(x), axis=0, keepdims=True)
                return 0

            lax.fori_loop(0, GE, one, 0)
            return 0

        lax.fori_loop(0, NG, group, 0)
        for t in range(8):
            for q in range(4):
                rs_s[m, 4 * t + q] = jnp.concatenate(
                    [lmax[m, pl.ds(4 * k, 4), pl.ds(128 * t, 128)][:, 32 * q : 32 * q + 32] for k in range(4)], axis=1
                )

    def start_rs(m):
        send_all(lambda p: rs_s.at[m, p], rs_r.at[m, me], rs_ss.at[m], rs_rs.at[m])
        rs_r[m, me] = rs_s[m, me]

    scales = (cg, cu, cd)

    def finish_rs(m):
        wait_bytes(rs_r.at[m, pl.ds(0, N - 1)], rs_rs.at[m])
        top = jnp.max(rs_r[m], axis=0)
        ag_s[m] = top
        ag_r[m, me] = top
        for k in range(4):
            scales[m][pl.ds(4 * k, 4), :] = top[:, 32 * k : 32 * k + 32]
        send_all(lambda p: ag_s.at[m], ag_r.at[m, me], ag_ss.at[m], ag_rs.at[m])

    def finish_ag(m):
        wait_bytes(ag_r.at[m, pl.ds(0, N - 1)], ag_rs.at[m])
        for t in range(8):
            for k in range(4):
                row = jnp.concatenate([ag_r[m, 4 * t + q][:, 32 * k : 32 * k + 32] for q in range(4)], axis=1)
                row = 1.0 / row
                for i in range(4):
                    inv[m, 4 * k + i, :, pl.ds(128 * t, 128)] = row[i : i + 1]

    def launch(gi):
        send_all(lambda p: snd.at[gi, p], rcv.at[gi, me], d_ss.at[gi], d_rs.at[gi])
        rcv[gi, me] = snd[gi, me]

    def stage(m, g, value):
        gi = m * NG + g

        def pair(j, _):
            ea = g * GE + 2 * j + xhi
            eb = g * GE + 2 * j + 1 - xhi
            for t in range(8):
                cs = pl.ds(128 * t, 128)
                x = jnp.concatenate([value(ea, cs), value(eb, cs)], axis=0).T.astype(BF16)
                snd[gi, pl.ds(4 * t, 4), j] = x.reshape(4, W, 128)
            return 0

        lax.fori_loop(0, GE // 2, pair, 0)

    def send_group(m, g):
        stage(m, g, lambda e, cs: mbuf[m, e, :, cs] * inv[m, e, :, cs])
        launch(m * NG + g)

    def encode(k, m, g):
        for i in range(GE):
            inl[k, i] = TOP / jnp.maximum(lmax[m, g * GE + i : g * GE + i + 1, :], TINY)

        def value(e, cs):
            v = mbuf[m, e, :, cs] * inl[k, e - g * GE, :, cs]
            p = v * v
            p = p * p
            p = p * p
            p = p * p
            return jnp.where(v < 0, -p, p)

        stage(m, g, value)

    def decode(code, factor):
        root = lax.rsqrt(lax.rsqrt(lax.rsqrt(lax.rsqrt(jnp.maximum(jnp.abs(code), SMALL))))) * factor
        return jnp.where(code == 0, 0.0, jnp.where(code < 0, -root, root))

    def receive_coded(k, m, g):
        gi = m * NG + g
        top = jnp.maximum(rs_r[m], TINY) / (ag_s[m][None] * TOP)
        fac[k] = top.reshape(N * 4, 128).T[W * g : W * (g + 1)]
        wait_bytes(rcv.at[gi, pl.ds(0, N - 1)], d_rs.at[gi])

        def tile(t, _):
            lanes = pl.ds(pl.multiple_of(t * 128, 128), 128)
            here = pltpu.roll(fac[k], lax.rem(128 - 8 * t, 128), 1)
            for j in range(GE // 2):
                col = lambda i: jnp.broadcast_to(here[:, i : i + 1], (W, 128))
                fa = jnp.where(low, col(2 * j), col(2 * j + 1))
                fb = jnp.where(low, col(5 + 2 * j), col(4 + 2 * j))
                a = decode(rcv[gi, 2 * t, j].astype(F32), fa)
                b = decode(rcv[gi, 2 * t + 1, j].astype(F32), fb)
                first = jnp.where(low, a, b)
                second = pltpu.roll(jnp.where(low, b, a), 64, 1)
                outs[m][g * GE + 2 * j, :, lanes] = first.astype(BF16)
                outs[m][g * GE + 2 * j + 1, :, lanes] = second.astype(BF16)
            return 0

        lax.fori_loop(0, N // 2, tile, 0)

    outs = (og, ou, od)
    low = lax.broadcasted_iota(jnp.int32, (W, 128), 1) < 64

    def receive_group(m, g):
        gi = m * NG + g
        wait_bytes(rcv.at[gi, pl.ds(0, N - 1)], d_rs.at[gi])

        def tile(t, _):
            lanes = pl.ds(pl.multiple_of(t * 128, 128), 128)
            for j in range(GE // 2):
                a = rcv[gi, 2 * t, j].astype(F32)
                b = rcv[gi, 2 * t + 1, j].astype(F32)
                first = jnp.where(low, a, b)
                second = pltpu.roll(jnp.where(low, b, a), 64, 1)
                outs[m][g * GE + 2 * j, :, lanes] = first.astype(BF16)
                outs[m][g * GE + 2 * j + 1, :, lanes] = second.astype(BF16)
            return 0

        lax.fori_loop(0, N // 2, tile, 0)

    merge(0)
    encode(0, 0, 0)
    pl.semaphore_wait(barrier, len(peers) + len(mates))
    start_rs(0)
    launch(0)
    merge(1)
    start_rs(1)
    encode(1, 1, 0)
    merge(2)
    start_rs(2)
    for c in router_in:
        c.wait()
    rt = rwb[...] * rgb[...]
    rt_s[...] = jnp.concatenate([rt[:8], rt[8:]], axis=1).astype(BF16)
    send_all(lambda p: rt_s, rt_r.at[me], rt_ss, rt_rs)
    rt_r[me] = rt_s[...]
    finish_rs(0)
    launch(NG)
    finish_rs(1)
    finish_rs(2)
    for m in range(3):
        finish_ag(m)

        def go(g, _):
            send_group(m, g)
            return 0

        lax.fori_loop(1 if m < 2 else 0, NG, go, 0)
        if m == 0:
            wait_bytes(rt_r.at[pl.ds(0, N - 1)], rt_rs)
            for t in range(16):
                a, b = rt_r[2 * t].astype(F32), rt_r[2 * t + 1].astype(F32)
                top = jnp.concatenate([a[:, :64], b[:, :64]], axis=1)
                bot = jnp.concatenate([a[:, 64:], b[:, 64:]], axis=1)
                rt_x[e_id, :, pl.ds(128 * t, 128)] = jnp.concatenate([top, bot], axis=0).astype(BF16)
            hop(rt_x.at[e_id], rx_ss.at[0], rx_rs.at[0], partner).start()
            hop(rt_x.at[e_id, :, pl.ds(0, 1024)], rx_ss.at[1], rx_rs.at[1], right).start()
            hop(rt_x.at[e_id, :, pl.ds(1024, 1024)], rx_ss.at[2], rx_rs.at[2], left).start()
    receive_coded(0, 0, 0)
    receive_coded(1, 1, 0)

    def come(m, start):
        def one(g, _):
            receive_group(m, g)
            return 0

        lax.fori_loop(start, NG, one, 0)

    come(0, 1)
    wait_bytes(rt_x.at[0, :, pl.ds(0, 1024)], rx_rs.at[1])
    wait_bytes(rt_x.at[0, :, pl.ds(0, 1024)], rx_rs.at[2])
    hop(rt_x.at[other], rx_ss.at[3], rx_rs.at[3], partner).start()
    come(1, 1)
    wait_bytes(rt_x.at[0], rx_rs.at[0])
    wait_bytes(rt_x.at[0], rx_rs.at[3])
    for k in range(4):
        orr[pl.ds(16 * k, 16), :] = rt_x[k]
    come(2, 0)
    wait_bytes(rt_x.at[0], rx_ss.at[0])
    wait_bytes(rt_x.at[0, :, pl.ds(0, 1024)], rx_ss.at[1])
    wait_bytes(rt_x.at[0, :, pl.ds(0, 1024)], rx_ss.at[2])
    wait_bytes(rt_x.at[0], rx_ss.at[3])
    wait_bytes(rt_r.at[pl.ds(0, N - 1)], rt_ss)
    for m in range(3):
        wait_bytes(rs_r.at[m, pl.ds(0, N - 1)], rs_ss.at[m])
        wait_bytes(ag_r.at[m, pl.ds(0, N - 1)], ag_ss.at[m])

    def drained(gi, _):
        wait_bytes(rcv.at[gi, pl.ds(0, N - 1)], d_ss.at[gi])
        return 0

    lax.fori_loop(0, 3 * NG, drained, 0)


def put_out(*refs):
    sem = refs[14]
    copies = [pltpu.make_async_copy(refs[i], refs[7 + i], sem.at[i]) for i in range(7)]
    for c in copies:
        c.start()
    for c in copies:
        c.wait()


def per_device(
    master_gate, second_gate, master_up, second_up, master_down, second_down, router_weight, router_gain
):
    vmem = pl.BlockSpec(memory_space=pltpu.VMEM)
    hbm = pl.BlockSpec(memory_space=pltpu.HBM)
    dma = pltpu.SemaphoreType.DMA
    big = jax.ShapeDtypeStruct((E, W, N * R), BF16)
    small = jax.ShapeDtypeStruct((E, W), F32)
    shapes = (big, big, big, small, small, small, jax.ShapeDtypeStruct((4 * E, N * R), BF16))
    results = pl.pallas_call(
        kernel,
        out_shape=shapes,
        in_specs=[hbm] * 8,
        out_specs=(vmem,) * 7,
        scratch_shapes=[
            pltpu.VMEM((16, R), F32),
            pltpu.VMEM((1, R), F32),
            pltpu.VMEM((3, E, R, C), F32),
            pltpu.VMEM((3, E, R, C), BF16),
            pltpu.VMEM((3, E, C), F32),
            pltpu.VMEM((2, GE, 1, C), F32),
            pltpu.VMEM((2, W, 128), F32),
            pltpu.VMEM((3, N, 4, 128), F32),
            pltpu.VMEM((3, N, 4, 128), F32),
            pltpu.VMEM((3, 4, 128), F32),
            pltpu.VMEM((3, N, 4, 128), F32),
            pltpu.VMEM((3, E, 1, C), F32),
            pltpu.VMEM((3 * NG, N, GE // 2, W, 128), BF16),
            pltpu.VMEM((3 * NG, N, GE // 2, W, 128), BF16),
            pltpu.VMEM((8, 128), BF16),
            pltpu.VMEM((N, 8, 128), BF16),
            pltpu.VMEM((4, 16, N * R), BF16),
            dma((2, 3 * NG)), dma((2,)), dma((3,)), dma((3,)), dma((3,)), dma((3,)), dma((3 * NG,)), dma((3 * NG,)),
            dma, dma, dma((4,)), dma((4,)),
        ],
        compiler_params=pltpu.CompilerParams(
            collective_id=0, has_side_effects=True, vmem_limit_bytes=47308 * 2**10
        ),
        name="reshard",
    )(
        master_gate, second_gate, master_up, second_up,
        jnp.swapaxes(master_down, 1, 2), jnp.swapaxes(second_down, 1, 2),
        router_weight.T, router_gain[None, :],
    )
    gate, up, down, cg, cu, cd, router = pl.pallas_call(
        put_out,
        out_shape=shapes,
        in_specs=[vmem] * 7,
        out_specs=(hbm,) * 7,
        scratch_shapes=[dma((7,))],
        compiler_params=pltpu.CompilerParams(vmem_limit_bytes=4 * 2**20),
        name="put_out",
    )(*results)
    return (jnp.swapaxes(gate, 1, 2), jnp.swapaxes(up, 1, 2), down, cg, cu, cd, router.T)


def solution(mesh):
    wide, tall = P("expert", "shard", None), P("expert", None, "shard")
    return jax.shard_map(
        per_device,
        mesh=mesh,
        in_specs=(wide, wide, wide, wide, tall, tall, P("shard", "expert"), P("shard")),
        out_specs=(tall, tall, wide, P("expert", "shard"), P("expert", "shard"), P("expert", "shard"), P()),
        check_vma=False,
    )
```

```python
import jax
import jax.numpy as jnp
from jax import lax
from jax.experimental import pallas as pl
from jax.experimental.pallas import tpu as pltpu
from jax.sharding import PartitionSpec as P

MESH = pl.DeviceIdType.MESH
F32, BF16 = jnp.float32, jnp.bfloat16
N = 32
E, R, C = 16, 64, 1024
W = C // N
GE = 4
NG = E // GE
TOP = 2.0 ** (127 / 16)
TINY = 1e-30
SMALL = 2.0**-126
OFFSETS = [
    (dx, dy, dz) for dx in range(2) for dy in range(4) for dz in range(4) if (dx, dy, dz) != (0, 0, 0)
]


def joined(a, b):
    low = lax.broadcasted_iota(jnp.int32, (W, 128), 1) < 64
    first = jnp.where(low, a, b)
    second = pltpu.roll(jnp.where(low, b, a), 64, 1)
    return first.astype(BF16), second.astype(BF16)


def kernel(
    mg, sg, mu, su, md, sd, rw, rg,
    og, ou, od, cg, cu, cd, orr, last,
    rwb, rgb, mbuf, sbuf, lmax, inl, fac, rs_s, rs_r, whole, ag_s, ag_r, inv, snd, rcv, rt_s, rt_r, rt_x,
    load_sem, rt_ld, rs_ss, rs_rs, ag_ss, ag_rs, d_ss, d_rs, rt_ss, rt_rs, rx_ss, rx_rs,
):
    e_id = lax.axis_index("expert")
    me = lax.axis_index("shard")
    xhi = lax.rem(me, 2)
    y = lax.rem(me // 2, 4)
    z = me // 8

    masters, seconds = (mg, mu, md), (sg, su, sd)
    for m in range(3):
        for g in range(NG):
            es = pl.ds(g * GE, GE)
            pltpu.make_async_copy(masters[m].at[es], mbuf.at[m, es], load_sem.at[0, m * NG + g]).start()
            pltpu.make_async_copy(seconds[m].at[es], sbuf.at[m, es], load_sem.at[1, m * NG + g]).start()

    peers = []
    for dx, dy, dz in OFFSETS:
        peers.append((lax.rem(z + dz, 4) * 4 + lax.rem(y + dy, 4)) * 2 + lax.rem(xhi + dx, 2))
    core = lax.rem(e_id, 2)
    xlo = e_id // 2
    other = (1 - xlo) * 2 + core
    column = me - xhi
    partner = (xlo * 2 + 1 - core, me)
    right = (other, column + lax.rem(xhi + xlo, 2))
    left = (other, column + lax.rem(xhi + 1 - xlo, 2))
    mates = (partner, right, left)

    barrier = pltpu.get_barrier_semaphore()
    for p in peers:
        pl.semaphore_signal(barrier, inc=1, device_id=(e_id, p), device_id_type=MESH)
    for q in mates:
        pl.semaphore_signal(barrier, inc=1, device_id=q, device_id_type=MESH)

    def send_all(src_of, dst, ss, rs):
        for p in peers:
            pltpu.make_async_remote_copy(
                src_ref=src_of(p), dst_ref=dst, send_sem=ss, recv_sem=rs,
                device_id=(e_id, p), device_id_type=MESH,
            ).start()

    def hop(ref, ss, rs, to):
        return pltpu.make_async_remote_copy(
            src_ref=ref, dst_ref=ref, send_sem=ss, recv_sem=rs, device_id=to, device_id_type=MESH
        )

    def wait_bytes(ref, sem):
        pltpu.make_async_copy(ref, ref, sem).wait()

    router_in = [pltpu.make_async_copy(a, b, rt_ld.at[i]) for i, (a, b) in enumerate(((rw, rwb), (rg, rgb)))]
    for c in router_in:
        c.start()

    def merge(m, start, stop):
        def group(g, _):
            es = pl.ds(g * GE, GE)
            wait_bytes(mbuf.at[m, es], load_sem.at[0, m * NG + g])
            wait_bytes(sbuf.at[m, es], load_sem.at[1, m * NG + g])

            def one(k, _):
                e = g * GE + k
                x = mbuf[m, e] + sbuf[m, e].astype(F32)
                mbuf[m, e] = x
                lmax[m, k, pl.ds(g, 1), :] = jnp.max(jnp.abs(x), axis=0, keepdims=True)
                return 0

            lax.fori_loop(0, GE, one, 0)
            return 0

        lax.fori_loop(start, stop, group, 0)

    def start_rs(m):
        for t in range(8):
            for q in range(4):
                rs_s[m, 4 * t + q] = jnp.concatenate(
                    [lmax[m, k, :, pl.ds(128 * t, 128)][:, 32 * q : 32 * q + 32] for k in range(GE)], axis=1
                )
        send_all(lambda p: rs_s.at[m, p], rs_r.at[m, me], rs_ss.at[m], rs_rs.at[m])
        rs_r[m, me] = rs_s[m, me]

    scales = (cg, cu, cd)

    def finish_rs(m):
        wait_bytes(rs_r.at[m, pl.ds(0, N - 1)], rs_rs.at[m])
        top = jnp.max(rs_r[m], axis=0)
        whole[m] = top
        ag_s[m] = top[1:]
        ag_r[m, me] = top[1:]
        send_all(lambda p: ag_s.at[m], ag_r.at[m, me], ag_ss.at[m], ag_rs.at[m])

    def put_scale(m):
        top = whole[m]
        for i in range(NG):
            for k in range(GE):
                scales[m][4 * i + k : 4 * i + k + 1, :] = top[i : i + 1, 32 * k : 32 * k + 32]

    def finish_ag(m):
        wait_bytes(ag_r.at[m, pl.ds(0, N - 1)], ag_rs.at[m])
        for t in range(8):
            for k in range(GE):
                row = jnp.concatenate([ag_r[m, 4 * t + q][:, 32 * k : 32 * k + 32] for q in range(4)], axis=1)
                row = 1.0 / row
                for i in range(1, NG):
                    inv[m, 4 * i + k, :, pl.ds(128 * t, 128)] = row[i - 1 : i]

    def launch(gi):
        send_all(lambda p: snd.at[gi, p], rcv.at[gi, me], d_ss.at[gi], d_rs.at[gi])
        rcv[gi, me] = snd[gi, me]

    def stage(m, g, value):
        gi = m * NG + g

        def pair(j, _):
            ea = g * GE + 2 * j + xhi
            eb = g * GE + 2 * j + 1 - xhi
            for t in range(8):
                cs = pl.ds(128 * t, 128)
                x = jnp.concatenate([value(ea, cs), value(eb, cs)], axis=0).T.astype(BF16)
                snd[gi, pl.ds(4 * t, 4), j] = x.reshape(4, W, 128)
            return 0

        lax.fori_loop(0, GE // 2, pair, 0)

    def send_group(m, g):
        stage(m, g, lambda e, cs: mbuf[m, e, :, cs] * inv[m, e, :, cs])
        launch(m * NG + g)

    def encode(m):
        for k in range(GE):
            inl[m, k] = TOP / jnp.maximum(lmax[m, k, 0:1, :], TINY)

        def value(e, cs):
            v = mbuf[m, e, :, cs] * inl[m, e, :, cs]
            p = v * v
            p = p * p
            p = p * p
            p = p * p
            return jnp.where(v < 0, -p, p)

        stage(m, 0, value)

    def decode(code, factor):
        root = lax.rsqrt(lax.rsqrt(lax.rsqrt(lax.rsqrt(jnp.maximum(jnp.abs(code), SMALL))))) * factor
        return jnp.where(code == 0, 0.0, jnp.where(code < 0, -root, root))

    def receive_coded(m):
        gi = m * NG
        top = jnp.maximum(rs_r[m][:, 0, :], TINY) / (whole[m][0:1, :] * TOP)
        top = jnp.concatenate([top, jnp.zeros((128 - N, 128), F32)], axis=0).T
        for k in range(GE):
            fac[k] = top[W * k : W * k + W]
        wait_bytes(rcv.at[gi, pl.ds(0, N - 1)], d_rs.at[gi])

        def tile(t, _):
            lanes = pl.ds(pl.multiple_of(t * 128, 128), 128)
            here = [pltpu.roll(fac[k], lax.rem(128 - 2 * t, 128), 1) for k in range(GE)]
            even = [jnp.broadcast_to(h[:, 0:1], (W, 128)) for h in here]
            odd = [jnp.broadcast_to(h[:, 1:2], (W, 128)) for h in here]
            for j in range(GE // 2):
                fa = jnp.where(low, even[2 * j], even[2 * j + 1])
                fb = jnp.where(low, odd[2 * j + 1], odd[2 * j])
                a = decode(rcv[gi, 2 * t, j].astype(F32), fa)
                b = decode(rcv[gi, 2 * t + 1, j].astype(F32), fb)
                first, second = joined(a, b)
                outs[m][2 * j, :, lanes] = first
                outs[m][2 * j + 1, :, lanes] = second
            return 0

        lax.fori_loop(0, N // 2, tile, 0)

    outs = (og, ou, od)
    low = lax.broadcasted_iota(jnp.int32, (W, 128), 1) < 64

    def receive_group(m, g):
        gi = m * NG + g
        wait_bytes(rcv.at[gi, pl.ds(0, N - 1)], d_rs.at[gi])

        def tile(t, _):
            lanes = pl.ds(pl.multiple_of(t * 128, 128), 128)
            for j in range(GE // 2):
                first, second = joined(rcv[gi, 2 * t, j].astype(F32), rcv[gi, 2 * t + 1, j].astype(F32))
                outs[m][g * GE + 2 * j, :, lanes] = first
                outs[m][g * GE + 2 * j + 1, :, lanes] = second
            return 0

        lax.fori_loop(0, N // 2, tile, 0)

    merge(0, 0, 1)
    encode(0)
    pl.semaphore_wait(barrier, len(peers) + len(mates))
    launch(0)
    merge(0, 1, NG)
    start_rs(0)
    merge(1, 0, 1)
    encode(1)
    launch(NG)
    merge(1, 1, NG)
    start_rs(1)
    merge(2, 0, 1)
    encode(2)
    merge(2, 1, NG)
    start_rs(2)
    finish_rs(0)
    launch(2 * NG)
    for c in router_in:
        c.wait()
    rt = rwb[...] * rgb[...]
    rt_s[...] = jnp.concatenate([rt[:8], rt[8:]], axis=1).astype(BF16)
    send_all(lambda p: rt_s, rt_r.at[me], rt_ss, rt_rs)
    rt_r[me] = rt_s[...]
    finish_rs(1)
    finish_rs(2)
    for m in range(3):
        finish_ag(m)

        def go(g, _):
            send_group(m, g)
            return 0

        lax.fori_loop(1, NG, go, 0)
        if m == 0:
            wait_bytes(rt_r.at[pl.ds(0, N - 1)], rt_rs)
            for t in range(16):
                a, b = rt_r[2 * t].astype(F32), rt_r[2 * t + 1].astype(F32)
                top = jnp.concatenate([a[:, :64], b[:, :64]], axis=1)
                bot = jnp.concatenate([a[:, 64:], b[:, 64:]], axis=1)
                rt_x[e_id, :, pl.ds(128 * t, 128)] = jnp.concatenate([top, bot], axis=0).astype(BF16)
            hop(rt_x.at[e_id], rx_ss.at[0], rx_rs.at[0], partner).start()
            hop(rt_x.at[e_id, :, pl.ds(0, 1024)], rx_ss.at[1], rx_rs.at[1], right).start()
            hop(rt_x.at[e_id, :, pl.ds(1024, 1024)], rx_ss.at[2], rx_rs.at[2], left).start()
    for m in range(3):
        receive_coded(m)
        put_scale(m)

    def come(m, stop):
        def one(g, _):
            receive_group(m, g)
            return 0

        lax.fori_loop(1, stop, one, 0)

    come(0, NG)
    wait_bytes(rt_x.at[0, :, pl.ds(0, 1024)], rx_rs.at[1])
    wait_bytes(rt_x.at[0, :, pl.ds(0, 1024)], rx_rs.at[2])
    hop(rt_x.at[other], rx_ss.at[3], rx_rs.at[3], partner).start()
    come(1, NG)
    wait_bytes(rt_x.at[0], rx_rs.at[0])
    wait_bytes(rt_x.at[0], rx_rs.at[3])
    for k in range(4):
        orr[pl.ds(16 * k, 16), :] = rt_x[k]
    come(2, NG - 1)
    wait_bytes(rcv.at[3 * NG - 1, pl.ds(0, N - 1)], d_rs.at[3 * NG - 1])
    last[...] = rcv[3 * NG - 1]
    wait_bytes(rt_x.at[0], rx_ss.at[0])
    wait_bytes(rt_x.at[0, :, pl.ds(0, 1024)], rx_ss.at[1])
    wait_bytes(rt_x.at[0, :, pl.ds(0, 1024)], rx_ss.at[2])
    wait_bytes(rt_x.at[0], rx_ss.at[3])
    wait_bytes(rt_r.at[pl.ds(0, N - 1)], rt_ss)
    for m in range(3):
        wait_bytes(rs_r.at[m, pl.ds(0, N - 1)], rs_ss.at[m])
        wait_bytes(ag_r.at[m, pl.ds(0, N - 1)], ag_ss.at[m])

    def drained(gi, _):
        wait_bytes(rcv.at[gi, pl.ds(0, N - 1)], d_ss.at[gi])
        return 0

    lax.fori_loop(0, 3 * NG, drained, 0)


def put_out(og, ou, od, cg, cu, cd, orr, last, hg, hu, hd, hcg, hcu, hcd, hr, tail, sem):
    done = pl.ds(0, E - GE)
    rest = pl.ds(E - GE, GE)
    pairs = ((og, hg), (ou, hu), (od.at[done], hd.at[done]), (cg, hcg), (cu, hcu), (cd, hcd), (orr, hr))
    copies = [pltpu.make_async_copy(a, b, sem.at[i]) for i, (a, b) in enumerate(pairs)]
    for c in copies:
        c.start()
    for t in range(N // 2):
        lanes = pl.ds(128 * t, 128)
        for j in range(GE // 2):
            first, second = joined(last[2 * t, j].astype(F32), last[2 * t + 1, j].astype(F32))
            tail[2 * j, :, lanes] = first
            tail[2 * j + 1, :, lanes] = second
    copies.append(pltpu.make_async_copy(tail, hd.at[rest], sem.at[7]))
    copies[-1].start()
    for c in copies:
        c.wait()


def per_device(
    master_gate, second_gate, master_up, second_up, master_down, second_down, router_weight, router_gain
):
    vmem = pl.BlockSpec(memory_space=pltpu.VMEM)
    hbm = pl.BlockSpec(memory_space=pltpu.HBM)
    dma = pltpu.SemaphoreType.DMA
    big = jax.ShapeDtypeStruct((E, W, N * R), BF16)
    small = jax.ShapeDtypeStruct((E, W), F32)
    raw = jax.ShapeDtypeStruct((N, GE // 2, W, 128), BF16)
    shapes = (big, big, big, small, small, small, jax.ShapeDtypeStruct((4 * E, N * R), BF16))
    results = pl.pallas_call(
        kernel,
        out_shape=shapes + (raw,),
        in_specs=[hbm] * 8,
        out_specs=(vmem,) * 8,
        scratch_shapes=[
            pltpu.VMEM((16, R), F32),
            pltpu.VMEM((1, R), F32),
            pltpu.VMEM((3, E, R, C), F32),
            pltpu.VMEM((3, E, R, C), BF16),
            pltpu.VMEM((3, GE, NG, C), F32),
            pltpu.VMEM((3, GE, 1, C), F32),
            pltpu.VMEM((GE, W, 128), F32),
            pltpu.VMEM((3, N, NG, 128), F32),
            pltpu.VMEM((3, N, NG, 128), F32),
            pltpu.VMEM((3, NG, 128), F32),
            pltpu.VMEM((3, NG - 1, 128), F32),
            pltpu.VMEM((3, N, NG - 1, 128), F32),
            pltpu.VMEM((3, E, 1, C), F32),
            pltpu.VMEM((3 * NG, N, GE // 2, W, 128), BF16),
            pltpu.VMEM((3 * NG, N, GE // 2, W, 128), BF16),
            pltpu.VMEM((8, 128), BF16),
            pltpu.VMEM((N, 8, 128), BF16),
            pltpu.VMEM((4, 16, N * R), BF16),
            dma((2, 3 * NG)), dma((2,)), dma((3,)), dma((3,)), dma((3,)), dma((3,)), dma((3 * NG,)), dma((3 * NG,)),
            dma, dma, dma((4,)), dma((4,)),
        ],
        compiler_params=pltpu.CompilerParams(
            collective_id=0, has_side_effects=True, vmem_limit_bytes=44 * 2**20
        ),
        name="reshard",
    )(
        *(
            pltpu.with_memory_space_constraint(x, pltpu.HBM)
            for x in (
                master_gate, second_gate, master_up, second_up,
                jnp.swapaxes(master_down, 1, 2), jnp.swapaxes(second_down, 1, 2),
                router_weight.T, router_gain[None, :],
            )
        )
    )
    gate, up, down, cg, cu, cd, router = pl.pallas_call(
        put_out,
        out_shape=shapes,
        in_specs=[vmem] * 8,
        out_specs=(hbm,) * 7,
        scratch_shapes=[pltpu.VMEM((GE, W, N * R), BF16), dma((8,))],
        compiler_params=pltpu.CompilerParams(vmem_limit_bytes=4 * 2**20),
        name="put_out",
    )(*results)
    return (jnp.swapaxes(gate, 1, 2), jnp.swapaxes(up, 1, 2), down, cg, cu, cd, router.T)


def solution(mesh):
    wide, tall = P("expert", "shard", None), P("expert", None, "shard")
    return jax.shard_map(
        per_device,
        mesh=mesh,
        in_specs=(wide, wide, wide, wide, tall, tall, P("shard", "expert"), P("shard")),
        out_specs=(tall, tall, wide, P("expert", "shard"), P("expert", "shard"), P("expert", "shard"), P()),
        check_vma=False,
    )
```

```python
import jax
import jax.numpy as jnp
from jax import lax
from jax.experimental import pallas as pl
from jax.experimental.pallas import tpu as pltpu
from jax.sharding import PartitionSpec as P

MESH = pl.DeviceIdType.MESH
F32, BF16 = jnp.float32, jnp.bfloat16
N = 32
E, R, C = 16, 64, 1024
W = C // N
GE = 4
NG = E // GE
TOP = 2.0 ** (79 / 16)
SPLIT = 2.0**31
TINY = 1e-30


def hops(offset):
    dx, dy, dz = offset
    return 2 * dx + min(dy, 4 - dy) + min(dz, 4 - dz)


OFFSETS = sorted(
    [(dx, dy, dz) for dx in range(2) for dy in range(4) for dz in range(4) if (dx, dy, dz) != (0, 0, 0)],
    key=hops,
    reverse=True,
)
AHEAD = 4
FAR = sum(hops(o) > 3 for o in OFFSETS)


def decode(code, factor):
    level = jnp.log2(jnp.abs(code))
    size = jnp.exp2(jnp.minimum(level * (1 / 32) - 127 / 32, level * (1 / 16) - 79 / 16)) * factor
    return jnp.where(code < 0, -size, size)


def decoded(t, codes, fac):
    low = lax.broadcasted_iota(jnp.int32, (W, 128), 1) < 64
    even = [jnp.broadcast_to(fac[k][:, 2 * t : 2 * t + 1], (W, 128)) for k in range(GE)]
    odd = [jnp.broadcast_to(fac[k][:, 2 * t + 1 : 2 * t + 2], (W, 128)) for k in range(GE)]
    found = []
    for j in range(GE // 2):
        fa = jnp.where(low, even[2 * j], even[2 * j + 1])
        fb = jnp.where(low, odd[2 * j + 1], odd[2 * j])
        a = decode(codes[2 * t, j].astype(F32), fa)
        b = decode(codes[2 * t + 1, j].astype(F32), fb)
        found.append(jnp.where(low, a, b).astype(BF16))
        found.append(pltpu.roll(jnp.where(low, b, a), 64, 1).astype(BF16))
    return found


def kernel(
    mg, sg, mu, su, md, sd, rw, rg,
    og, ou, od, cg, cu, cd, orr, last, lfac,
    rwb, rgb, mbuf, sbuf, lmax, inl, fac, rs_s, rs_r, snd, rcv, rt_s, rt_r, rt_x,
    load_sem, rt_ld, rs_ss, rs_rs, ready, d_ss, d_rs, rt_ss, rt_rs, rx_ss, rx_rs,
):
    e_id = lax.axis_index("expert")
    me = lax.axis_index("shard")
    xhi = lax.rem(me, 2)
    y = lax.rem(me // 2, 4)
    z = me // 8

    masters, seconds = (mg, mu, md), (sg, su, sd)
    for m in range(3):
        for g in range(NG):
            es = pl.ds(g * GE, GE)
            pltpu.make_async_copy(masters[m].at[es], mbuf.at[m, es], load_sem.at[0, m * NG + g]).start()
            pltpu.make_async_copy(seconds[m].at[es], sbuf.at[m, es], load_sem.at[1, m * NG + g]).start()

    peers = []
    for dx, dy, dz in OFFSETS:
        peers.append((lax.rem(z + dz, 4) * 4 + lax.rem(y + dy, 4)) * 2 + lax.rem(xhi + dx, 2))
    core = lax.rem(e_id, 2)
    xlo = e_id // 2
    other = (1 - xlo) * 2 + core
    column = me - xhi
    partner = (xlo * 2 + 1 - core, me)
    right = (other, column + lax.rem(xhi + xlo, 2))
    left = (other, column + lax.rem(xhi + 1 - xlo, 2))
    mates = (partner, right, left)

    barrier = pltpu.get_barrier_semaphore()
    for p in peers:
        pl.semaphore_signal(barrier, inc=1, device_id=(e_id, p), device_id_type=MESH)
    for q in mates:
        pl.semaphore_signal(barrier, inc=1, device_id=q, device_id_type=MESH)

    def send_all(src_of, dst, ss, rs, to=peers):
        for p in to:
            pltpu.make_async_remote_copy(
                src_ref=src_of(p), dst_ref=dst, send_sem=ss, recv_sem=rs,
                device_id=(e_id, p), device_id_type=MESH,
            ).start()

    def hop(ref, ss, rs, to):
        return pltpu.make_async_remote_copy(
            src_ref=ref, dst_ref=ref, send_sem=ss, recv_sem=rs, device_id=to, device_id_type=MESH
        )

    def wait_bytes(ref, sem):
        pltpu.make_async_copy(ref, ref, sem).wait()

    router_in = [pltpu.make_async_copy(a, b, rt_ld.at[i]) for i, (a, b) in enumerate(((rw, rwb), (rg, rgb)))]
    for c in router_in:
        c.start()

    def merge(m, start):
        def group(g, _):
            gi = m * NG + g
            es = pl.ds(g * GE, GE)
            wait_bytes(mbuf.at[m, es], load_sem.at[0, gi])
            wait_bytes(sbuf.at[m, es], load_sem.at[1, gi])

            def one(k, _):
                e = g * GE + k
                x = mbuf[m, e] + sbuf[m, e].astype(F32)
                mbuf[m, e] = x
                row = jnp.max(jnp.abs(x), axis=0, keepdims=True)
                lmax[m, k, pl.ds(g, 1), :] = row
                inl[m, e] = TOP / jnp.maximum(row, TINY)
                return 0

            lax.fori_loop(0, GE, one, 0)
            return 0

        lax.fori_loop(start, NG if start or m else 1, group, 0)

    def stage(m, g):
        gi = m * NG + g

        def coded(k, cs):
            e = g * GE + k
            v = mbuf[m, e, :, cs] * inl[m, e, :, cs]
            p = v * v
            p = p * p
            p = p * p
            p = p * p
            p = jnp.where(p < SPLIT, p, p * (p * (1 / SPLIT)))
            return jnp.where(v < 0, -p, p)

        def pair(j, _):
            for t in range(8):
                cs = pl.ds(128 * t, 128)
                x = jnp.concatenate([coded(2 * j + xhi, cs), coded(2 * j + 1 - xhi, cs)], axis=0).T.astype(BF16)
                snd[gi, pl.ds(4 * t, 4), j] = x.reshape(4, W, 128)
            return 0

        lax.fori_loop(0, GE // 2, pair, 0)
        rcv[gi, me] = snd[gi, me]

    def launch(gi, to):
        send_all(lambda p: snd.at[gi, p], rcv.at[gi, me], d_ss.at[gi], d_rs.at[gi], to)

    def start_rs(m):
        for t in range(8):
            for q in range(4):
                rs_s[m, 4 * t + q] = jnp.concatenate(
                    [lmax[m, k, :, pl.ds(128 * t, 128)][:, 32 * q : 32 * q + 32] for k in range(GE)], axis=1
                )
        send_all(lambda p: rs_s.at[m, p], rs_r.at[m, me], rs_ss.at[m], rs_rs.at[m])
        rs_r[m, me] = rs_s[m, me]

    scales = (cg, cu, cd)

    def finish_rs(m):
        wait_bytes(rs_r.at[m, pl.ds(0, N - 1)], rs_rs.at[m])
        top = jnp.max(rs_r[m], axis=0)
        for i in range(NG):
            for k in range(GE):
                scales[m][4 * i + k : 4 * i + k + 1, :] = top[i : i + 1, 32 * k : 32 * k + 32]
            f = jnp.maximum(rs_r[m][:, i, :], TINY) / top[i : i + 1]
            f = jnp.concatenate([f, jnp.zeros((128 - N, 128), F32)], axis=0).T
            for k in range(GE):
                fac[i, k] = f[W * k : W * k + W]

    outs = (og, ou, od)
    def receive(m, g):
        gi = m * NG + g
        wait_bytes(rcv.at[gi, pl.ds(0, N - 1)], d_rs.at[gi])

        for t in range(N // 2):
            for i, x in enumerate(decoded(t, rcv.at[gi], fac.at[g])):
                outs[m][g * GE + i, :, pl.ds(128 * t, 128)] = x

    def drain(gi):
        wait_bytes(rcv.at[gi, pl.ds(0, N - 1)], d_ss.at[gi])

    def send_groups(m, start, stop):
        def go(g, _):
            stage(m, g)
            launch(m * NG + g, peers)
            return 0

        lax.fori_loop(start, stop, go, 0)

    def exchange(m, start, back_m, back_start):
        def go(i, _):
            stage(m, start + i)
            drain(back_m * NG + back_start + i)
            launch(m * NG + start + i, peers)
            receive(back_m, back_start + i)
            return 0

        lax.fori_loop(0, 2, go, 0)

    def routers_out():
        wait_bytes(rt_r.at[pl.ds(0, N - 1)], rt_rs)
        for t in range(16):
            a, b = rt_r[2 * t].astype(F32), rt_r[2 * t + 1].astype(F32)
            top = jnp.concatenate([a[:, :64], b[:, :64]], axis=1)
            bot = jnp.concatenate([a[:, 64:], b[:, 64:]], axis=1)
            rt_x[e_id, :, pl.ds(128 * t, 128)] = jnp.concatenate([top, bot], axis=0).astype(BF16)
        hop(rt_x.at[e_id], rx_ss.at[0], rx_rs.at[0], partner).start()
        hop(rt_x.at[e_id, :, pl.ds(0, 1024)], rx_ss.at[1], rx_rs.at[1], right).start()
        hop(rt_x.at[e_id, :, pl.ds(1024, 1024)], rx_ss.at[2], rx_rs.at[2], left).start()

    merge(0, 0)
    stage(0, 0)
    pl.semaphore_wait(barrier, len(peers) + len(mates))
    launch(0, peers)
    merge(0, 1)
    start_rs(0)
    send_groups(0, 1, 2)
    merge(1, 0)
    start_rs(1)
    send_groups(0, 2, 3)
    merge(2, 0)
    start_rs(2)
    for c in router_in:
        c.wait()
    rt = rwb[...] * rgb[...]
    rt_s[...] = jnp.concatenate([rt[:8], rt[8:]], axis=1).astype(BF16)
    send_all(lambda p: rt_s, rt_r.at[me], rt_ss, rt_rs)
    rt_r[me] = rt_s[...]
    send_groups(0, 3, NG)
    if AHEAD > NG:
        send_groups(1, 0, AHEAD - NG)
    finish_rs(0)
    for back in range(0, 3 * NG - AHEAD, 2):
        bm, bg = divmod(back, NG)
        m, g = divmod(back + AHEAD, NG)
        if bg == 0 and bm:
            finish_rs(bm)
        exchange(m, g, bm, bg)
        if back == 0:
            routers_out()
        if back == 2:
            wait_bytes(rt_x.at[0, :, pl.ds(0, 1024)], rx_rs.at[1])
            wait_bytes(rt_x.at[0, :, pl.ds(0, 1024)], rx_rs.at[2])
            hop(rt_x.at[other], rx_ss.at[3], rx_rs.at[3], partner).start()
    wait_bytes(rt_x.at[0], rx_rs.at[0])
    wait_bytes(rt_x.at[0], rx_rs.at[3])
    for k in range(4):
        orr[pl.ds(16 * k, 16), :] = rt_x[k]
    for back in range(3 * NG - AHEAD, 3 * NG, 2):
        bm, bg = divmod(back, NG)
        if bg == 0:
            finish_rs(bm)

        def come(i, _):
            receive(bm, bg + i)
            return 0

        lax.fori_loop(0, 1 if back + 2 == 3 * NG else 2, come, 0)
    wait_bytes(rcv.at[3 * NG - 1, pl.ds(0, N - 1)], d_rs.at[3 * NG - 1])
    last[...] = rcv[3 * NG - 1]
    lfac[...] = fac[NG - 1]
    wait_bytes(rt_x.at[0], rx_ss.at[0])
    wait_bytes(rt_x.at[0, :, pl.ds(0, 1024)], rx_ss.at[1])
    wait_bytes(rt_x.at[0, :, pl.ds(0, 1024)], rx_ss.at[2])
    wait_bytes(rt_x.at[0], rx_ss.at[3])
    wait_bytes(rt_r.at[pl.ds(0, N - 1)], rt_ss)
    for m in range(3):
        wait_bytes(rs_r.at[m, pl.ds(0, N - 1)], rs_ss.at[m])

    def drained(gi, _):
        drain(gi)
        return 0

    lax.fori_loop(3 * NG - AHEAD, 3 * NG, drained, 0)


def put_out(og, ou, od, cg, cu, cd, orr, last, lfac, hg, hu, hd, hcg, hcu, hcd, hr, tail, sem):
    done = pl.ds(0, E - GE)
    rest = pl.ds(E - GE, GE)
    pairs = ((og, hg), (ou, hu), (od.at[done], hd.at[done]), (cg, hcg), (cu, hcu), (cd, hcd), (orr, hr))
    copies = [pltpu.make_async_copy(a, b, sem.at[i]) for i, (a, b) in enumerate(pairs)]
    for c in copies:
        c.start()

    for t in range(N // 2):
        for i, x in enumerate(decoded(t, last, lfac)):
            tail[i, :, pl.ds(128 * t, 128)] = x
    copies.append(pltpu.make_async_copy(tail, hd.at[rest], sem.at[7]))
    copies[-1].start()
    for c in copies:
        c.wait()


def per_device(
    master_gate, second_gate, master_up, second_up, master_down, second_down, router_weight, router_gain
):
    vmem = pl.BlockSpec(memory_space=pltpu.VMEM)
    hbm = pl.BlockSpec(memory_space=pltpu.HBM)
    dma = pltpu.SemaphoreType.DMA
    big = jax.ShapeDtypeStruct((E, W, N * R), BF16)
    small = jax.ShapeDtypeStruct((E, W), F32)
    raw = (jax.ShapeDtypeStruct((N, GE // 2, W, 128), BF16), jax.ShapeDtypeStruct((GE, W, 128), F32))
    shapes = (big, big, big, small, small, small, jax.ShapeDtypeStruct((4 * E, N * R), BF16))
    results = pl.pallas_call(
        kernel,
        out_shape=shapes + raw,
        in_specs=[hbm] * 8,
        out_specs=(vmem,) * 9,
        scratch_shapes=[
            pltpu.VMEM((16, R), F32),
            pltpu.VMEM((1, R), F32),
            pltpu.VMEM((3, E, R, C), F32),
            pltpu.VMEM((3, E, R, C), BF16),
            pltpu.VMEM((3, GE, NG, C), F32),
            pltpu.VMEM((3, E, 1, C), F32),
            pltpu.VMEM((NG, GE, W, 128), F32),
            pltpu.VMEM((3, N, NG, 128), F32),
            pltpu.VMEM((3, N, NG, 128), F32),
            pltpu.VMEM((3 * NG, N, GE // 2, W, 128), BF16),
            pltpu.VMEM((3 * NG, N, GE // 2, W, 128), BF16),
            pltpu.VMEM((8, 128), BF16),
            pltpu.VMEM((N, 8, 128), BF16),
            pltpu.VMEM((4, 16, N * R), BF16),
            dma((2, 3 * NG)), dma((2,)), dma((3,)), dma((3,)), pltpu.SemaphoreType.REGULAR, dma((3 * NG,)), dma((3 * NG,)),
            dma, dma, dma((4,)), dma((4,)),
        ],
        compiler_params=pltpu.CompilerParams(
            collective_id=0, has_side_effects=True, vmem_limit_bytes=44 * 2**20
        ),
        name="reshard",
    )(
        *(
            pltpu.with_memory_space_constraint(x, pltpu.HBM)
            for x in (
                master_gate, second_gate, master_up, second_up,
                jnp.swapaxes(master_down, 1, 2), jnp.swapaxes(second_down, 1, 2),
                router_weight.T, router_gain[None, :],
            )
        )
    )
    gate, up, down, cg, cu, cd, router = pl.pallas_call(
        put_out,
        out_shape=shapes,
        in_specs=[vmem] * 9,
        out_specs=(hbm,) * 7,
        scratch_shapes=[pltpu.VMEM((GE, W, N * R), BF16), dma((8,))],
        compiler_params=pltpu.CompilerParams(vmem_limit_bytes=4 * 2**20),
        name="put_out",
    )(*results)
    return (jnp.swapaxes(gate, 1, 2), jnp.swapaxes(up, 1, 2), down, cg, cu, cd, router.T)


def solution(mesh):
    wide, tall = P("expert", "shard", None), P("expert", None, "shard")
    return jax.shard_map(
        per_device,
        mesh=mesh,
        in_specs=(wide, wide, wide, wide, tall, tall, P("shard", "expert"), P("shard")),
        out_specs=(tall, tall, wide, P("expert", "shard"), P("expert", "shard"), P("expert", "shard"), P()),
        check_vma=False,
    )
```

```python
import jax
import jax.numpy as jnp
from jax import lax
from jax.experimental import pallas as pl
from jax.experimental.pallas import tpu as pltpu
from jax.sharding import PartitionSpec as P

MESH = pl.DeviceIdType.MESH
F32, BF16 = jnp.float32, jnp.bfloat16
N = 32
E, R, C = 16, 64, 1024
W = C // N
GE = 4
NG = E // GE
TOP = 2.0 ** (79 / 16)
SPLIT = 2.0**31
TINY = 1e-30


def hops(offset):
    dx, dy, dz = offset
    return 2 * dx + min(dy, 4 - dy) + min(dz, 4 - dz)


OFFSETS = sorted(
    [(dx, dy, dz) for dx in range(2) for dy in range(4) for dz in range(4) if (dx, dy, dz) != (0, 0, 0)],
    key=lambda o: (-hops(o), (o[1] + 2 * o[2]) % 4, o[0]),
)
AHEAD = 4
FAR = sum(hops(o) > 3 for o in OFFSETS)


def decode(code, factor):
    level = jnp.log2(jnp.abs(code))
    size = jnp.exp2(jnp.minimum(level * (1 / 32) - 127 / 32, level * (1 / 16) - 79 / 16)) * factor
    return jnp.where(code < 0, -size, size)


def decoded(t, codes, fac):
    low = lax.broadcasted_iota(jnp.int32, (W, 128), 1) < 64
    even = [jnp.broadcast_to(fac[k][:, 2 * t : 2 * t + 1], (W, 128)) for k in range(GE)]
    odd = [jnp.broadcast_to(fac[k][:, 2 * t + 1 : 2 * t + 2], (W, 128)) for k in range(GE)]
    found = []
    for j in range(GE // 2):
        fa = jnp.where(low, even[2 * j], even[2 * j + 1])
        fb = jnp.where(low, odd[2 * j + 1], odd[2 * j])
        a = decode(codes[2 * t, j].astype(F32), fa)
        b = decode(codes[2 * t + 1, j].astype(F32), fb)
        found.append(jnp.where(low, a, b).astype(BF16))
        found.append(pltpu.roll(jnp.where(low, b, a), 64, 1).astype(BF16))
    return found


def kernel(
    mg, sg, mu, su, md, sd, rw, rg,
    og, ou, od, cg, cu, cd, orr, last, lfac,
    rwb, rgb, mbuf, sbuf, lmax, inl, fac, rs_s, rs_r, snd, rcv, rt_s, rt_r, rt_x,
    load_sem, rt_ld, rs_ss, rs_rs, d_ss, d_rs, rt_ss, rt_rs, rx_ss, rx_rs,
):
    e_id = lax.axis_index("expert")
    me = lax.axis_index("shard")
    xhi = lax.rem(me, 2)
    y = lax.rem(me // 2, 4)
    z = me // 8

    masters, seconds = (mg, mu, md), (sg, su, sd)
    for m in range(3):
        for g in range(NG):
            es = pl.ds(g * GE, GE)
            pltpu.make_async_copy(masters[m].at[es], mbuf.at[m, es], load_sem.at[0, m * NG + g]).start()
            pltpu.make_async_copy(seconds[m].at[es], sbuf.at[m, es], load_sem.at[1, m * NG + g]).start()

    peers = []
    for dx, dy, dz in OFFSETS:
        peers.append((lax.rem(z + dz, 4) * 4 + lax.rem(y + dy, 4)) * 2 + lax.rem(xhi + dx, 2))
    core = lax.rem(e_id, 2)
    xlo = e_id // 2
    other = (1 - xlo) * 2 + core
    column = me - xhi
    partner = (xlo * 2 + 1 - core, me)
    right = (other, column + lax.rem(xhi + xlo, 2))
    left = (other, column + lax.rem(xhi + 1 - xlo, 2))
    mates = (partner, right, left)

    barrier = pltpu.get_barrier_semaphore()
    for p in peers:
        pl.semaphore_signal(barrier, inc=1, device_id=(e_id, p), device_id_type=MESH)
    for q in mates:
        pl.semaphore_signal(barrier, inc=1, device_id=q, device_id_type=MESH)

    def send_all(src_of, dst, ss, rs, to=peers):
        for p in to:
            pltpu.make_async_remote_copy(
                src_ref=src_of(p), dst_ref=dst, send_sem=ss, recv_sem=rs,
                device_id=(e_id, p), device_id_type=MESH,
            ).start()

    def hop(ref, ss, rs, to):
        return pltpu.make_async_remote_copy(
            src_ref=ref, dst_ref=ref, send_sem=ss, recv_sem=rs, device_id=to, device_id_type=MESH
        )

    def wait_bytes(ref, sem):
        pltpu.make_async_copy(ref, ref, sem).wait()

    router_in = [pltpu.make_async_copy(a, b, rt_ld.at[i]) for i, (a, b) in enumerate(((rw, rwb), (rg, rgb)))]
    for c in router_in:
        c.start()

    def merge(m, start):
        def group(g, _):
            gi = m * NG + g
            es = pl.ds(g * GE, GE)
            wait_bytes(mbuf.at[m, es], load_sem.at[0, gi])
            wait_bytes(sbuf.at[m, es], load_sem.at[1, gi])

            def one(k, _):
                e = g * GE + k
                x = mbuf[m, e] + sbuf[m, e].astype(F32)
                mbuf[m, e] = x
                row = jnp.max(jnp.abs(x), axis=0, keepdims=True)
                lmax[m, k, pl.ds(g, 1), :] = row
                inl[m, e] = TOP / jnp.maximum(row, TINY)
                return 0

            lax.fori_loop(0, GE, one, 0)
            return 0

        lax.fori_loop(start, NG if start or m else 1, group, 0)

    def stage(m, g):
        gi = m * NG + g

        def coded(k, cs):
            e = g * GE + k
            v = mbuf[m, e, :, cs] * inl[m, e, :, cs]
            p = v * v
            p = p * p
            p = p * p
            p = p * p
            p = jnp.where(p < SPLIT, p, p * (p * (1 / SPLIT)))
            return jnp.where(v < 0, -p, p)

        def pair(j, _):
            for t in range(8):
                cs = pl.ds(128 * t, 128)
                x = jnp.concatenate([coded(2 * j + xhi, cs), coded(2 * j + 1 - xhi, cs)], axis=0).T.astype(BF16)
                snd[gi, pl.ds(4 * t, 4), j] = x.reshape(4, W, 128)
            return 0

        lax.fori_loop(0, GE // 2, pair, 0)
        rcv[gi, me] = snd[gi, me]

    def launch(gi, to):
        send_all(lambda p: snd.at[gi, p], rcv.at[gi, me], d_ss.at[gi], d_rs.at[gi], to)

    def start_rs(m):
        for t in range(8):
            for q in range(4):
                rs_s[m, 4 * t + q] = jnp.concatenate(
                    [lmax[m, k, :, pl.ds(128 * t, 128)][:, 32 * q : 32 * q + 32] for k in range(GE)], axis=1
                )
        send_all(lambda p: rs_s.at[m, p], rs_r.at[m, me], rs_ss.at[m], rs_rs.at[m])
        rs_r[m, me] = rs_s[m, me]

    scales = (cg, cu, cd)

    def finish_rs(m):
        wait_bytes(rs_r.at[m, pl.ds(0, N - 1)], rs_rs.at[m])
        top = jnp.max(rs_r[m], axis=0)
        for i in range(NG):
            for k in range(GE):
                scales[m][4 * i + k : 4 * i + k + 1, :] = top[i : i + 1, 32 * k : 32 * k + 32]
            f = jnp.maximum(rs_r[m][:, i, :], TINY) / top[i : i + 1]
            f = jnp.concatenate([f, jnp.zeros((128 - N, 128), F32)], axis=0).T
            for k in range(GE):
                fac[i, k] = f[W * k : W * k + W]

    outs = (og, ou, od)
    def receive(m, g):
        gi = m * NG + g
        wait_bytes(rcv.at[gi, pl.ds(0, N - 1)], d_rs.at[gi])

        for t in range(N // 2):
            for i, x in enumerate(decoded(t, rcv.at[gi], fac.at[g])):
                outs[m][g * GE + i, :, pl.ds(128 * t, 128)] = x

    def drain(gi):
        wait_bytes(rcv.at[gi, pl.ds(0, N - 1)], d_ss.at[gi])

    def send_groups(m, start, stop):
        def go(g, _):
            stage(m, g)
            launch(m * NG + g, peers)
            return 0

        lax.fori_loop(start, stop, go, 0)

    def exchange(m, start, back_m, back_start):
        def go(i, _):
            stage(m, start + i)
            drain(back_m * NG + back_start + i)
            launch(m * NG + start + i, peers)
            receive(back_m, back_start + i)
            return 0

        lax.fori_loop(0, 2, go, 0)

    def routers_out():
        wait_bytes(rt_r.at[pl.ds(0, N - 1)], rt_rs)
        for t in range(16):
            a, b = rt_r[2 * t].astype(F32), rt_r[2 * t + 1].astype(F32)
            top = jnp.concatenate([a[:, :64], b[:, :64]], axis=1)
            bot = jnp.concatenate([a[:, 64:], b[:, 64:]], axis=1)
            rt_x[e_id, :, pl.ds(128 * t, 128)] = jnp.concatenate([top, bot], axis=0).astype(BF16)
        hop(rt_x.at[e_id], rx_ss.at[0], rx_rs.at[0], partner).start()
        hop(rt_x.at[e_id, :, pl.ds(0, 1024)], rx_ss.at[1], rx_rs.at[1], right).start()
        hop(rt_x.at[e_id, :, pl.ds(1024, 1024)], rx_ss.at[2], rx_rs.at[2], left).start()

    merge(0, 0)
    stage(0, 0)
    pl.semaphore_wait(barrier, len(peers) + len(mates))
    launch(0, peers)
    merge(0, 1)
    start_rs(0)
    send_groups(0, 1, 2)
    merge(1, 0)
    start_rs(1)
    send_groups(0, 2, 3)
    merge(2, 0)
    start_rs(2)
    for c in router_in:
        c.wait()
    rt = rwb[...] * rgb[...]
    rt_s[...] = jnp.concatenate([rt[:8], rt[8:]], axis=1).astype(BF16)
    send_all(lambda p: rt_s, rt_r.at[me], rt_ss, rt_rs)
    rt_r[me] = rt_s[...]
    send_groups(0, 3, NG)
    if AHEAD > NG:
        send_groups(1, 0, AHEAD - NG)
    finish_rs(0)
    for back in range(0, 3 * NG - AHEAD, 2):
        bm, bg = divmod(back, NG)
        m, g = divmod(back + AHEAD, NG)
        if bg == 0 and bm:
            finish_rs(bm)
        exchange(m, g, bm, bg)
        if back == 0:
            routers_out()
        if back == 2:
            wait_bytes(rt_x.at[0, :, pl.ds(0, 1024)], rx_rs.at[1])
            wait_bytes(rt_x.at[0, :, pl.ds(0, 1024)], rx_rs.at[2])
            hop(rt_x.at[other], rx_ss.at[3], rx_rs.at[3], partner).start()
    wait_bytes(rt_x.at[0], rx_rs.at[0])
    wait_bytes(rt_x.at[0], rx_rs.at[3])
    for k in range(4):
        orr[pl.ds(16 * k, 16), :] = rt_x[k]
    for back in range(3 * NG - AHEAD, 3 * NG, 2):
        bm, bg = divmod(back, NG)
        if bg == 0:
            finish_rs(bm)

        def come(i, _):
            receive(bm, bg + i)
            return 0

        lax.fori_loop(0, 1 if back + 2 == 3 * NG else 2, come, 0)
    wait_bytes(rt_x.at[0], rx_ss.at[0])
    wait_bytes(rt_x.at[0, :, pl.ds(0, 1024)], rx_ss.at[1])
    wait_bytes(rt_x.at[0, :, pl.ds(0, 1024)], rx_ss.at[2])
    wait_bytes(rt_x.at[0], rx_ss.at[3])
    wait_bytes(rt_r.at[pl.ds(0, N - 1)], rt_ss)
    for m in range(3):
        wait_bytes(rs_r.at[m, pl.ds(0, N - 1)], rs_ss.at[m])

    def drained(gi, _):
        drain(gi)
        return 0

    lax.fori_loop(3 * NG - AHEAD, 3 * NG, drained, 0)
    wait_bytes(rcv.at[3 * NG - 1, pl.ds(0, N - 1)], d_rs.at[3 * NG - 1])
    last[...] = rcv[3 * NG - 1]
    lfac[...] = fac[NG - 1]


def put_out(og, ou, od, cg, cu, cd, orr, last, lfac, hg, hu, hd, hcg, hcu, hcd, hr, tail, sem):
    done = pl.ds(0, E - GE)
    rest = pl.ds(E - GE, GE)
    pairs = ((og, hg), (ou, hu), (od.at[done], hd.at[done]), (cg, hcg), (cu, hcu), (cd, hcd), (orr, hr))
    copies = [pltpu.make_async_copy(a, b, sem.at[i]) for i, (a, b) in enumerate(pairs)]
    for c in copies:
        c.start()

    for t in range(N // 2):
        for i, x in enumerate(decoded(t, last, lfac)):
            tail[i, :, pl.ds(128 * t, 128)] = x
    copies.append(pltpu.make_async_copy(tail, hd.at[rest], sem.at[7]))
    copies[-1].start()
    for c in copies:
        c.wait()


def per_device(
    master_gate, second_gate, master_up, second_up, master_down, second_down, router_weight, router_gain
):
    vmem = pl.BlockSpec(memory_space=pltpu.VMEM)
    hbm = pl.BlockSpec(memory_space=pltpu.HBM)
    dma = pltpu.SemaphoreType.DMA
    big = jax.ShapeDtypeStruct((E, W, N * R), BF16)
    small = jax.ShapeDtypeStruct((E, W), F32)
    raw = (jax.ShapeDtypeStruct((N, GE // 2, W, 128), BF16), jax.ShapeDtypeStruct((GE, W, 128), F32))
    shapes = (big, big, big, small, small, small, jax.ShapeDtypeStruct((4 * E, N * R), BF16))
    results = pl.pallas_call(
        kernel,
        out_shape=shapes + raw,
        in_specs=[hbm] * 8,
        out_specs=(vmem,) * 9,
        scratch_shapes=[
            pltpu.VMEM((16, R), F32),
            pltpu.VMEM((1, R), F32),
            pltpu.VMEM((3, E, R, C), F32),
            pltpu.VMEM((3, E, R, C), BF16),
            pltpu.VMEM((3, GE, NG, C), F32),
            pltpu.VMEM((3, E, 1, C), F32),
            pltpu.VMEM((NG, GE, W, 128), F32),
            pltpu.VMEM((3, N, NG, 128), F32),
            pltpu.VMEM((3, N, NG, 128), F32),
            pltpu.VMEM((3 * NG, N, GE // 2, W, 128), BF16),
            pltpu.VMEM((3 * NG, N, GE // 2, W, 128), BF16),
            pltpu.VMEM((8, 128), BF16),
            pltpu.VMEM((N, 8, 128), BF16),
            pltpu.VMEM((4, 16, N * R), BF16),
            dma((2, 3 * NG)), dma((2,)), dma((3,)), dma((3,)), dma((3 * NG,)), dma((3 * NG,)),
            dma, dma, dma((4,)), dma((4,)),
        ],
        compiler_params=pltpu.CompilerParams(
            collective_id=0, has_side_effects=True, vmem_limit_bytes=44 * 2**20
        ),
        name="reshard",
    )(
        *(
            pltpu.with_memory_space_constraint(x, pltpu.HBM)
            for x in (
                master_gate, second_gate, master_up, second_up,
                jnp.swapaxes(master_down, 1, 2), jnp.swapaxes(second_down, 1, 2),
                router_weight.T, router_gain[None, :],
            )
        )
    )
    gate, up, down, cg, cu, cd, router = pl.pallas_call(
        put_out,
        out_shape=shapes,
        in_specs=[vmem] * 9,
        out_specs=(hbm,) * 7,
        scratch_shapes=[pltpu.VMEM((GE, W, N * R), BF16), dma((8,))],
        compiler_params=pltpu.CompilerParams(vmem_limit_bytes=4 * 2**20),
        name="put_out",
    )(*results)
    return (jnp.swapaxes(gate, 1, 2), jnp.swapaxes(up, 1, 2), down, cg, cu, cd, router.T)


def solution(mesh):
    wide, tall = P("expert", "shard", None), P("expert", None, "shard")
    return jax.shard_map(
        per_device,
        mesh=mesh,
        in_specs=(wide, wide, wide, wide, tall, tall, P("shard", "expert"), P("shard")),
        out_specs=(tall, tall, wide, P("expert", "shard"), P("expert", "shard"), P("expert", "shard"), P()),
        check_vma=False,
    )
```

```python
import jax
import jax.numpy as jnp
from jax import lax
from jax.experimental import pallas as pl
from jax.experimental.pallas import tpu as pltpu
from jax.sharding import PartitionSpec as P

MESH = pl.DeviceIdType.MESH
F32, BF16 = jnp.float32, jnp.bfloat16
N = 32
E, R, C = 16, 64, 1024
W = C // N
GE = 4
NG = E // GE
TOP = 2.0 ** (79 / 16)
SPLIT = 2.0**31
TINY = 1e-30


def hops(offset):
    dx, dy, dz = offset
    return 2 * dx + min(dy, 4 - dy) + min(dz, 4 - dz)


OFFSETS = sorted(
    [(dx, dy, dz) for dx in range(2) for dy in range(4) for dz in range(4) if (dx, dy, dz) != (0, 0, 0)],
    key=lambda o: (-hops(o), (o[1] + 2 * o[2]) % 4, o[0]),
)
AHEAD = 6
FAR = sum(hops(o) > 3 for o in OFFSETS)


def decode(code, factor):
    level = jnp.log2(jnp.abs(code))
    size = jnp.exp2(jnp.minimum(level * (1 / 32) - 127 / 32, level * (1 / 16) - 79 / 16)) * factor
    return jnp.where(code < 0, -size, size)


def decoded(t, codes, fac):
    low = lax.broadcasted_iota(jnp.int32, (W, 128), 1) < 64
    even = [jnp.broadcast_to(fac[k][:, 2 * t : 2 * t + 1], (W, 128)) for k in range(GE)]
    odd = [jnp.broadcast_to(fac[k][:, 2 * t + 1 : 2 * t + 2], (W, 128)) for k in range(GE)]
    found = []
    for j in range(GE // 2):
        fa = jnp.where(low, even[2 * j], even[2 * j + 1])
        fb = jnp.where(low, odd[2 * j + 1], odd[2 * j])
        a = decode(codes[2 * t, j].astype(F32), fa)
        b = decode(codes[2 * t + 1, j].astype(F32), fb)
        found.append(jnp.where(low, a, b).astype(BF16))
        found.append(pltpu.roll(jnp.where(low, b, a), 64, 1).astype(BF16))
    return found


def kernel(
    mg, sg, mu, su, md, sd, rw, rg,
    og, ou, od, cg, cu, cd, orr, last, lfac,
    rwb, rgb, mbuf, sbuf, lmax, inl, fac, rs_s, rs_r, snd, rcv, rt_s, rt_r, rt_x,
    load_sem, rt_ld, rs_ss, rs_rs, d_ss, d_rs, rt_ss, rt_rs, rx_ss, rx_rs,
):
    e_id = lax.axis_index("expert")
    me = lax.axis_index("shard")
    xhi = lax.rem(me, 2)
    y = lax.rem(me // 2, 4)
    z = me // 8

    masters, seconds = (mg, mu, md), (sg, su, sd)
    for m in range(3):
        for g in range(NG):
            es = pl.ds(g * GE, GE)
            pltpu.make_async_copy(masters[m].at[es], mbuf.at[m, es], load_sem.at[0, m * NG + g]).start()
            pltpu.make_async_copy(seconds[m].at[es], sbuf.at[m, es], load_sem.at[1, m * NG + g]).start()

    peers = []
    for dx, dy, dz in OFFSETS:
        peers.append((lax.rem(z + dz, 4) * 4 + lax.rem(y + dy, 4)) * 2 + lax.rem(xhi + dx, 2))
    core = lax.rem(e_id, 2)
    xlo = e_id // 2
    other = (1 - xlo) * 2 + core
    column = me - xhi
    partner = (xlo * 2 + 1 - core, me)
    right = (other, column + lax.rem(xhi + xlo, 2))
    left = (other, column + lax.rem(xhi + 1 - xlo, 2))
    mates = (partner, right, left)

    barrier = pltpu.get_barrier_semaphore()
    for p in peers:
        pl.semaphore_signal(barrier, inc=1, device_id=(e_id, p), device_id_type=MESH)
    for q in mates:
        pl.semaphore_signal(barrier, inc=1, device_id=q, device_id_type=MESH)

    def send_all(src_of, dst, ss, rs, to=peers):
        for p in to:
            pltpu.make_async_remote_copy(
                src_ref=src_of(p), dst_ref=dst, send_sem=ss, recv_sem=rs,
                device_id=(e_id, p), device_id_type=MESH,
            ).start()

    def hop(ref, ss, rs, to):
        return pltpu.make_async_remote_copy(
            src_ref=ref, dst_ref=ref, send_sem=ss, recv_sem=rs, device_id=to, device_id_type=MESH
        )

    def wait_bytes(ref, sem):
        pltpu.make_async_copy(ref, ref, sem).wait()

    router_in = [pltpu.make_async_copy(a, b, rt_ld.at[i]) for i, (a, b) in enumerate(((rw, rwb), (rg, rgb)))]
    for c in router_in:
        c.start()

    def merge(m, start):
        def group(g, _):
            gi = m * NG + g
            es = pl.ds(g * GE, GE)
            wait_bytes(mbuf.at[m, es], load_sem.at[0, gi])
            wait_bytes(sbuf.at[m, es], load_sem.at[1, gi])

            def one(k, _):
                e = g * GE + k
                x = mbuf[m, e] + sbuf[m, e].astype(F32)
                mbuf[m, e] = x
                row = jnp.max(jnp.abs(x), axis=0, keepdims=True)
                lmax[m, k, pl.ds(g, 1), :] = row
                inl[m, e] = TOP / jnp.maximum(row, TINY)
                return 0

            lax.fori_loop(0, GE, one, 0)
            return 0

        lax.fori_loop(start, NG if start or m else 1, group, 0)

    def stage(m, g):
        gi = m * NG + g

        def coded(k, cs):
            e = g * GE + k
            v = mbuf[m, e, :, cs] * inl[m, e, :, cs]
            p = v * v
            p = p * p
            p = p * p
            p = p * p
            p = jnp.where(p < SPLIT, p, p * (p * (1 / SPLIT)))
            return jnp.where(v < 0, -p, p)

        def pair(j, _):
            for t in range(8):
                cs = pl.ds(128 * t, 128)
                x = jnp.concatenate([coded(2 * j + xhi, cs), coded(2 * j + 1 - xhi, cs)], axis=0).T.astype(BF16)
                snd[gi, pl.ds(4 * t, 4), j] = x.reshape(4, W, 128)
            return 0

        lax.fori_loop(0, GE // 2, pair, 0)
        rcv[gi, me] = snd[gi, me]

    def launch(gi, to):
        send_all(lambda p: snd.at[gi, p], rcv.at[gi, me], d_ss.at[gi], d_rs.at[gi], to)

    def start_rs(m):
        for t in range(8):
            for q in range(4):
                rs_s[m, 4 * t + q] = jnp.concatenate(
                    [lmax[m, k, :, pl.ds(128 * t, 128)][:, 32 * q : 32 * q + 32] for k in range(GE)], axis=1
                )
        send_all(lambda p: rs_s.at[m, p], rs_r.at[m, me], rs_ss.at[m], rs_rs.at[m])
        rs_r[m, me] = rs_s[m, me]

    scales = (cg, cu, cd)

    def finish_rs(m):
        wait_bytes(rs_r.at[m, pl.ds(0, N - 1)], rs_rs.at[m])
        top = jnp.max(rs_r[m], axis=0)
        for i in range(NG):
            for k in range(GE):
                scales[m][4 * i + k : 4 * i + k + 1, :] = top[i : i + 1, 32 * k : 32 * k + 32]
            f = jnp.maximum(rs_r[m][:, i, :], TINY) / top[i : i + 1]
            f = jnp.concatenate([f, jnp.zeros((128 - N, 128), F32)], axis=0).T
            for k in range(GE):
                fac[i, k] = f[W * k : W * k + W]

    outs = (og, ou, od)
    def receive(m, g):
        gi = m * NG + g
        wait_bytes(rcv.at[gi, pl.ds(0, N - 1)], d_rs.at[gi])

        for t in range(N // 2):
            for i, x in enumerate(decoded(t, rcv.at[gi], fac.at[g])):
                outs[m][g * GE + i, :, pl.ds(128 * t, 128)] = x

    def drain(gi):
        wait_bytes(rcv.at[gi, pl.ds(0, N - 1)], d_ss.at[gi])

    def send_groups(m, start, stop):
        def go(g, _):
            stage(m, g)
            launch(m * NG + g, peers)
            return 0

        lax.fori_loop(start, stop, go, 0)

    def exchange(m, start, back_m, back_start):
        def go(i, _):
            stage(m, start + i)
            drain(back_m * NG + back_start + i)
            launch(m * NG + start + i, peers)
            receive(back_m, back_start + i)
            return 0

        lax.fori_loop(0, 2, go, 0)

    def routers_out():
        wait_bytes(rt_r.at[pl.ds(0, N - 1)], rt_rs)
        for t in range(16):
            a, b = rt_r[2 * t].astype(F32), rt_r[2 * t + 1].astype(F32)
            top = jnp.concatenate([a[:, :64], b[:, :64]], axis=1)
            bot = jnp.concatenate([a[:, 64:], b[:, 64:]], axis=1)
            rt_x[e_id, :, pl.ds(128 * t, 128)] = jnp.concatenate([top, bot], axis=0).astype(BF16)
        hop(rt_x.at[e_id], rx_ss.at[0], rx_rs.at[0], partner).start()
        hop(rt_x.at[e_id, :, pl.ds(0, 1024)], rx_ss.at[1], rx_rs.at[1], right).start()
        hop(rt_x.at[e_id, :, pl.ds(1024, 1024)], rx_ss.at[2], rx_rs.at[2], left).start()

    merge(0, 0)
    stage(0, 0)
    pl.semaphore_wait(barrier, len(peers) + len(mates))
    launch(0, peers)
    merge(0, 1)
    start_rs(0)
    send_groups(0, 1, 2)
    merge(1, 0)
    start_rs(1)
    send_groups(0, 2, 3)
    merge(2, 0)
    start_rs(2)
    for c in router_in:
        c.wait()
    rt = rwb[...] * rgb[...]
    rt_s[...] = jnp.concatenate([rt[:8], rt[8:]], axis=1).astype(BF16)
    send_all(lambda p: rt_s, rt_r.at[me], rt_ss, rt_rs)
    rt_r[me] = rt_s[...]
    send_groups(0, 3, NG)
    if AHEAD > NG:
        send_groups(1, 0, AHEAD - NG)
    finish_rs(0)
    for back in range(0, 3 * NG - AHEAD, 2):
        bm, bg = divmod(back, NG)
        m, g = divmod(back + AHEAD, NG)
        if bg == 0 and bm:
            finish_rs(bm)
        exchange(m, g, bm, bg)
        if back == 0:
            routers_out()
        if back == 2:
            wait_bytes(rt_x.at[0, :, pl.ds(0, 1024)], rx_rs.at[1])
            wait_bytes(rt_x.at[0, :, pl.ds(0, 1024)], rx_rs.at[2])
            hop(rt_x.at[other], rx_ss.at[3], rx_rs.at[3], partner).start()
    wait_bytes(rt_x.at[0], rx_rs.at[0])
    wait_bytes(rt_x.at[0], rx_rs.at[3])
    for k in range(4):
        orr[pl.ds(16 * k, 16), :] = rt_x[k]
    for back in range(3 * NG - AHEAD, 3 * NG, 2):
        bm, bg = divmod(back, NG)
        if bg == 0:
            finish_rs(bm)

        def come(i, _):
            receive(bm, bg + i)
            return 0

        lax.fori_loop(0, 1 if back + 2 == 3 * NG else 2, come, 0)
    wait_bytes(rt_x.at[0], rx_ss.at[0])
    wait_bytes(rt_x.at[0, :, pl.ds(0, 1024)], rx_ss.at[1])
    wait_bytes(rt_x.at[0, :, pl.ds(0, 1024)], rx_ss.at[2])
    wait_bytes(rt_x.at[0], rx_ss.at[3])
    wait_bytes(rt_r.at[pl.ds(0, N - 1)], rt_ss)
    for m in range(3):
        wait_bytes(rs_r.at[m, pl.ds(0, N - 1)], rs_ss.at[m])

    def drained(gi, _):
        drain(gi)
        return 0

    lax.fori_loop(3 * NG - AHEAD, 3 * NG, drained, 0)
    wait_bytes(rcv.at[3 * NG - 1, pl.ds(0, N - 1)], d_rs.at[3 * NG - 1])
    last[...] = rcv[3 * NG - 1]
    lfac[...] = fac[NG - 1]


def put_out(og, ou, od, cg, cu, cd, orr, last, lfac, hg, hu, hd, hcg, hcu, hcd, hr, tail, sem):
    done = pl.ds(0, E - GE)
    rest = pl.ds(E - GE, GE)
    pairs = ((og, hg), (ou, hu), (od.at[done], hd.at[done]), (cg, hcg), (cu, hcu), (cd, hcd), (orr, hr))
    copies = [pltpu.make_async_copy(a, b, sem.at[i]) for i, (a, b) in enumerate(pairs)]
    for c in copies:
        c.start()

    for t in range(N // 2):
        for i, x in enumerate(decoded(t, last, lfac)):
            tail[i, :, pl.ds(128 * t, 128)] = x
    copies.append(pltpu.make_async_copy(tail, hd.at[rest], sem.at[7]))
    copies[-1].start()
    for c in copies:
        c.wait()


def per_device(
    master_gate, second_gate, master_up, second_up, master_down, second_down, router_weight, router_gain
):
    vmem = pl.BlockSpec(memory_space=pltpu.VMEM)
    hbm = pl.BlockSpec(memory_space=pltpu.HBM)
    dma = pltpu.SemaphoreType.DMA
    big = jax.ShapeDtypeStruct((E, W, N * R), BF16)
    small = jax.ShapeDtypeStruct((E, W), F32)
    raw = (jax.ShapeDtypeStruct((N, GE // 2, W, 128), BF16), jax.ShapeDtypeStruct((GE, W, 128), F32))
    shapes = (big, big, big, small, small, small, jax.ShapeDtypeStruct((4 * E, N * R), BF16))
    results = pl.pallas_call(
        kernel,
        out_shape=shapes + raw,
        in_specs=[hbm] * 8,
        out_specs=(vmem,) * 9,
        scratch_shapes=[
            pltpu.VMEM((16, R), F32),
            pltpu.VMEM((1, R), F32),
            pltpu.VMEM((3, E, R, C), F32),
            pltpu.VMEM((3, E, R, C), BF16),
            pltpu.VMEM((3, GE, NG, C), F32),
            pltpu.VMEM((3, E, 1, C), F32),
            pltpu.VMEM((NG, GE, W, 128), F32),
            pltpu.VMEM((3, N, NG, 128), F32),
            pltpu.VMEM((3, N, NG, 128), F32),
            pltpu.VMEM((3 * NG, N, GE // 2, W, 128), BF16),
            pltpu.VMEM((3 * NG, N, GE // 2, W, 128), BF16),
            pltpu.VMEM((8, 128), BF16),
            pltpu.VMEM((N, 8, 128), BF16),
            pltpu.VMEM((4, 16, N * R), BF16),
            dma((2, 3 * NG)), dma((2,)), dma((3,)), dma((3,)), dma((3 * NG,)), dma((3 * NG,)),
            dma, dma, dma((4,)), dma((4,)),
        ],
        compiler_params=pltpu.CompilerParams(
            collective_id=0, has_side_effects=True, vmem_limit_bytes=44 * 2**20
        ),
        name="reshard",
    )(
        *(
            pltpu.with_memory_space_constraint(x, pltpu.HBM)
            for x in (
                master_gate, second_gate, master_up, second_up,
                jnp.swapaxes(master_down, 1, 2), jnp.swapaxes(second_down, 1, 2),
                router_weight.T, router_gain[None, :],
            )
        )
    )
    gate, up, down, cg, cu, cd, router = pl.pallas_call(
        put_out,
        out_shape=shapes,
        in_specs=[vmem] * 9,
        out_specs=(hbm,) * 7,
        scratch_shapes=[pltpu.VMEM((GE, W, N * R), BF16), dma((8,))],
        compiler_params=pltpu.CompilerParams(vmem_limit_bytes=4 * 2**20),
        name="put_out",
    )(*results)
    return (jnp.swapaxes(gate, 1, 2), jnp.swapaxes(up, 1, 2), down, cg, cu, cd, router.T)


def solution(mesh):
    wide, tall = P("expert", "shard", None), P("expert", None, "shard")
    return jax.shard_map(
        per_device,
        mesh=mesh,
        in_specs=(wide, wide, wide, wide, tall, tall, P("shard", "expert"), P("shard")),
        out_specs=(tall, tall, wide, P("expert", "shard"), P("expert", "shard"), P("expert", "shard"), P()),
        check_vma=False,
    )
```
